8 devices in a mesh: dp: 1 (over z), sx: 2 (over y), sy: 4 (over x, core).
Axes of the slice: x: 2, y: 2, z: 1, core: 2. Of those that a mesh axis runs over, the one named last changes fastest.
Arguments:
- act_in: bfloat16 [16, 1024, 16, 256], P('dp', 'sy', 'sx')
- norm_first: bfloat16 [2, 256], replicated
- w_first: bfloat16 [3, 3, 256, 128], replicated
- w_short: bfloat16 [256, 128], replicated
- norm_rest: bfloat16 [6, 2, 128], replicated
- w_rest: bfloat16 [5, 3, 3, 128, 128], replicated
- bias_rest: bfloat16 [7, 128], replicated
- w_out: bfloat16 [3, 3, 128, 3], replicated
- bias_out: bfloat16 [3], replicated
Outputs:
- output: float32 [16, 1024, 16, 3], P('dp', 'sy', 'sx')
All inputs are finite; a program needn't handle non-finite values.
Results may differ from the reference program's by a relative error of at most 0.00879114.
Values are sent between devices in bfloat16 or wider.
A program may use at most 1 GiB of HBM per device.

```python
import math
import jax
import jax.numpy as jnp
from jax import lax

SAMPLES = 16
IMG_H = 1024
IMG_W = 16
IN_CH = 256
MID_CH = 128
OUT_CH = 3
GROUPS = 32
GN_EPS = 1e-6


def normal_weight(key, shape, fan_in):
    return (jax.random.normal(key, shape, jnp.float32) * fan_in ** -0.5).astype(jnp.bfloat16)


def norm_params(key, layer_count, chan_count):
    gain_key, shift_key = jax.random.split(key)
    gains = 1.0 + 0.25 * jax.random.normal(gain_key, (layer_count, chan_count), jnp.float32)
    shifts = 0.25 * jax.random.normal(shift_key, (layer_count, chan_count), jnp.float32)
    return jnp.stack([gains, shifts], axis=1).astype(jnp.bfloat16)


def setup_inputs(seed: int = 0, part: int = 0) -> dict:
    base_key = jax.random.key(seed)
    act_keys = jax.random.split(jax.random.fold_in(base_key, part), 6)
    weight_keys = jax.random.split(base_key, 8)
    wave_count = 3
    base_noise = jax.random.normal(act_keys[0], (SAMPLES, IMG_H, IMG_W, IN_CH), jnp.float32)
    wave_amp = jax.random.normal(act_keys[1], (SAMPLES, wave_count, 1, IN_CH), jnp.float32)
    row_freq = jax.random.uniform(act_keys[2], (SAMPLES, wave_count, 1, 1), jnp.float32, 0.5, 2.5)
    col_freq = jax.random.uniform(act_keys[3], (SAMPLES, wave_count, 1, 1), jnp.float32, 0.5, 2.5)
    row_phase = jax.random.uniform(act_keys[4], (SAMPLES, wave_count, 1, IN_CH), jnp.float32, 0.0, 2.0 * math.pi)
    col_phase = jax.random.uniform(act_keys[5], (SAMPLES, wave_count, 1, IN_CH), jnp.float32, 0.0, 2.0 * math.pi)
    row_pos = (jnp.arange(IMG_H, dtype=jnp.float32) / IMG_H)[:, None]
    col_pos = (jnp.arange(IMG_W, dtype=jnp.float32) / IMG_W)[:, None]
    row_wave = wave_amp * jnp.cos(2.0 * math.pi * row_freq * row_pos + row_phase)
    col_wave = jnp.cos(2.0 * math.pi * col_freq * col_pos + col_phase)
    smooth_field = jnp.einsum("skhc,skwc->shwc", row_wave, col_wave)
    act_in = (0.7 * base_noise + smooth_field).astype(jnp.bfloat16)
    return {
        "act_in": act_in,
        "norm_first": norm_params(weight_keys[0], 1, IN_CH)[0],
        "w_first": normal_weight(weight_keys[1], (3, 3, IN_CH, MID_CH), 9 * IN_CH),
        "w_short": normal_weight(weight_keys[2], (IN_CH, MID_CH), IN_CH),
        "norm_rest": norm_params(weight_keys[3], 6, MID_CH),
        "w_rest": normal_weight(weight_keys[4], (5, 3, 3, MID_CH, MID_CH), 9 * MID_CH),
        "bias_rest": (0.3 * jax.random.normal(weight_keys[5], (7, MID_CH), jnp.float32)).astype(jnp.bfloat16),
        "w_out": normal_weight(weight_keys[6], (3, 3, MID_CH, OUT_CH), 9 * MID_CH),
        "bias_out": (0.3 * jax.random.normal(weight_keys[7], (OUT_CH,), jnp.float32)).astype(jnp.bfloat16),
    }


def group_norm_act(act_map, norm_pair):
    num_rows, num_cols, channels = act_map.shape
    per_group = channels // GROUPS
    group_count = num_rows * num_cols * per_group
    sum_one = jnp.sum(act_map, axis=(0, 1), dtype=jnp.float32).reshape(GROUPS, per_group).sum(axis=1)
    sum_two = jnp.sum(jnp.square(act_map.astype(jnp.float32)), axis=(0, 1)).reshape(GROUPS, per_group).sum(axis=1)
    group_mean = sum_one / group_count
    inv_std = lax.rsqrt(sum_two / group_count - group_mean * group_mean + GN_EPS)
    chan_scale = jnp.repeat(inv_std, per_group) * norm_pair[0].astype(jnp.float32)
    chan_shift = norm_pair[1].astype(jnp.float32) - jnp.repeat(group_mean, per_group) * chan_scale
    return jax.nn.silu(act_map.astype(jnp.float32) * chan_scale + chan_shift).astype(jnp.bfloat16)


def conv_three(act_map, kernel):
    num_rows, num_cols, in_chans = act_map.shape
    padded = jnp.pad(act_map, ((1, 1), (1, 1), (0, 0)))
    accum_sum = jnp.zeros((num_rows * num_cols, kernel.shape[3]), jnp.float32)
    for row_off in range(3):
        for col_off in range(3):
            window = padded[row_off:row_off + num_rows, col_off:col_off + num_cols].reshape(num_rows * num_cols, in_chans)
            accum_sum = accum_sum + jnp.dot(window, kernel[row_off, col_off], preferred_element_type=jnp.float32)
    return accum_sum.reshape(num_rows, num_cols, kernel.shape[3])


def reference(act_in, norm_first, w_first, w_short, norm_rest, w_rest, bias_rest, w_out, bias_out):
    bias_rows = bias_rest.astype(jnp.float32)

    def decode_sample(sample):
        num_rows, num_cols, in_chans = sample.shape
        mid_act = (conv_three(group_norm_act(sample, norm_first), w_first) + bias_rows[0]).astype(jnp.bfloat16)
        skip_path = jnp.dot(sample.reshape(num_rows * num_cols, in_chans), w_short, preferred_element_type=jnp.float32).reshape(num_rows, num_cols, -1) + bias_rows[6]
        hidden = (conv_three(group_norm_act(mid_act, norm_rest[0]), w_rest[0]) + bias_rows[1] + skip_path).astype(jnp.bfloat16)
        for res_index in range(1, 3):
            first_at = 2 * res_index - 1
            mid_act = (conv_three(group_norm_act(hidden, norm_rest[first_at]), w_rest[first_at]) + bias_rows[first_at + 1]).astype(jnp.bfloat16)
            hidden = (conv_three(group_norm_act(mid_act, norm_rest[first_at + 1]), w_rest[first_at + 1]) + bias_rows[first_at + 2] + hidden.astype(jnp.float32)).astype(jnp.bfloat16)
        return conv_three(group_norm_act(hidden, norm_rest[5]), w_out) + bias_out.astype(jnp.float32)

    return lax.map(decode_sample, act_in)
```

```python
import jax
import jax.numpy as jnp
from jax import lax
from jax.experimental import pallas as pl
from jax.experimental.pallas import tpu as pltpu
from jax.sharding import PartitionSpec as P

MESH = pl.DeviceIdType.MESH
GN_EPS = 1e-6
NG = 4
NS = 4
SUB = 16
J = 8
BC = 8
RC = 8
RB = 4
LAYERS = 7


def solution(mesh):
    tile_spec = P("dp", "sy", "sx", None)
    rep = P()

    def kernel(a_hbm, w1_ref, wr_ref, ws_ref, wo_ref, nrm_ref, bias_ref, y_ref,
               a_buf, t_buf, h_buf, cola, colx, rowa, rowx, cora, corx, act, wp1, wp2, wpr, wpo,
               raw, tmp, sacc, stat_own, stat_in, sb,
               raw_sem, col_s, col_r, row_s, row_r, cor_s, cor_r, st_s, st_r):
        sx = lax.axis_index("sx")
        sy = lax.axis_index("sy")
        px = 1 - sx
        up = lax.rem(sy + 3, 4)
        dn = lax.rem(sy + 1, 4)
        me = sx * 4 + sy
        R = a_buf.shape[1]
        count = 1024.0 * 16.0

        def peer(d):
            other = lax.rem(me + d, 8)
            return {"sx": lax.div(other, 4), "sy": lax.rem(other, 4)}

        barrier = pltpu.get_barrier_semaphore()
        for d in range(1, 8):
            pl.semaphore_signal(barrier, inc=1, device_id=peer(d), device_id_type=MESH)

        def raw_copy(g, chunk, slot):
            return pltpu.make_async_copy(
                a_hbm.at[pl.ds(g * NS, NS), :, pl.ds(chunk * RC, RC)], raw.at[slot], raw_sem.at[slot])

        nchunk = R // RC
        raw_copy(0, 0, 0).start()

        def rcopy(src, dst, ss, rs, dev):
            return pltpu.make_async_remote_copy(src_ref=src, dst_ref=dst, send_sem=ss, recv_sem=rs, device_id=dev, device_id_type=MESH)

        def xbuf(l):
            return a_buf if l == 0 else (t_buf if l % 2 else h_buf)

        def halo_copies(l, g):
            x = xbuf(l)
            if l == 0:
                col, row, cor = cola.at[g], rowa.at[g], cora.at[g]
            else:
                col, row, cor = colx.at[l % 2, g], rowx.at[l % 2, g], corx.at[l % 2, g]
            return [
                rcopy(x.at[g, R - 1], row.at[0], row_s.at[l, g, 0], row_r.at[l, g, 0], {"sx": sx, "sy": dn}),
                rcopy(x.at[g, 0], row.at[1], row_s.at[l, g, 1], row_r.at[l, g, 1], {"sx": sx, "sy": up}),
                rcopy(x.at[g, R - 1, 0], cor.at[0], cor_s.at[l, g, 0], cor_r.at[l, g, 0], {"sx": px, "sy": dn}),
                rcopy(x.at[g, 0, 0], cor.at[1], cor_s.at[l, g, 1], cor_r.at[l, g, 1], {"sx": px, "sy": up}),
                rcopy(x.at[g, :, 0], col, col_s.at[l, g], col_r.at[l, g], {"sx": px, "sy": sy}),
            ]

        def stat_copies(l, g):
            nh = 2 if l == 0 else 1
            return [
                rcopy(stat_own.at[l % 2, g, pl.ds(0, nh)], stat_in.at[l % 2, g, d - 1, pl.ds(0, nh)],
                      st_s.at[l, g, d - 1], st_r.at[l, g, d - 1], peer(d))
                for d in range(1, 8)
            ]

        sub8 = lax.broadcasted_iota(jnp.int32, (8, 128), 0)
        lane8 = lax.broadcasted_iota(jnp.int32, (8, 128), 1)

        def fold(v):
            v = v[0:8] + v[8:16]
            return v + pltpu.roll(v, 4, 0)

        def push_stats(l, g):
            for half in range(2 if l == 0 else 1):
                one = fold(sacc[0, half])
                two = fold(sacc[1, half])
                stat_own[l % 2, g, half] = jnp.where(sub8 < 4, one, two)
            for c in stat_copies(l, g):
                c.start()

        def zero_stats():
            sacc[...] = jnp.zeros_like(sacc)

        def load_group(g, _):
            zero_stats()

            def load_chunk(ch, _):
                step = g * nchunk + ch
                slot = lax.rem(step, 2)
                nxt = step + 1

                @pl.when(nxt < NG * nchunk)
                def _():
                    raw_copy(lax.div(nxt, nchunk), lax.rem(nxt, nchunk), lax.rem(nxt, 2)).start()

                raw_copy(g, ch, slot).wait()
                ones = [jnp.zeros((SUB, 128), jnp.float32) for _ in range(2)]
                twos = [jnp.zeros((SUB, 128), jnp.float32) for _ in range(2)]
                for r in range(RC):
                    for p in range(NG):
                        for i in range(NS):
                            v = raw[slot, i, p, r].astype(jnp.float32)
                            base = (p * NS + i) * J
                            tmp[r % 2, 0, base:base + J, :] = v[:, :128]
                            tmp[r % 2, 1, base:base + J, :] = v[:, 128:]
                    for w in range(J):
                        j = sx * w + (1 - sx) * (J - 1 - w)
                        for half in range(2):
                            v = tmp[r % 2, half, pl.ds(w, SUB, stride=J), :]
                            a_buf[g, ch * RC + r, j, :, half * 128:(half + 1) * 128] = v.astype(jnp.bfloat16)
                            ones[half] = ones[half] + v
                            twos[half] = twos[half] + v * v
                for half in range(2):
                    sacc[0, half] = sacc[0, half] + ones[half]
                    sacc[1, half] = sacc[1, half] + twos[half]
                return 0

            lax.fori_loop(0, nchunk, load_chunk, 0)

            @pl.when(g == 0)
            def _():
                pl.semaphore_wait(barrier, 7)

            push_stats(0, g)
            for c in halo_copies(0, g):
                c.start()
            return 0

        lax.fori_loop(0, NG, load_group, 0)

        def fill_pairs(dst, get, ch):
            zero = jnp.zeros((ch, 128), jnp.bfloat16)
            for dy in range(3):
                for d4 in range(4):
                    k = (dy * 4 + d4) * ch
                    dst[k:k + ch, 0:128] = get(dy, d4) if d4 < 3 else zero
                    dst[k:k + ch, 128:256] = get(dy, d4 - 1) if d4 > 0 else zero

        def real_dx(dx):
            return sx * dx + (1 - sx) * (2 - dx)

        fill_pairs(wp1, lambda dy, dx: w1_ref[dy, real_dx(dx)], 256)
        fill_pairs(wp2, lambda dy, dx: wr_ref[0, dy, real_dx(dx)], 128)
        zs = jnp.zeros((256, 128), jnp.bfloat16)
        wp2[1536:1792, 0:128] = ws_ref[...]
        wp2[1536:1792, 128:256] = zs
        wp2[1792:2048, 0:128] = zs
        wp2[1792:2048, 128:256] = ws_ref[...]
        for k in range(1, 5):
            fill_pairs(wpr.at[k - 1], lambda dy, dx, k=k: wr_ref[k, dy, real_dx(dx)], 128)

        lane128 = lax.broadcasted_iota(jnp.int32, (128, 128), 1)

        def fill_out(c, _):
            wpad = sx * c + (1 - sx) * (J + 1 - c)
            placed = []
            for dy in range(3):
                rolled = pltpu.roll(wo_ref[dy], lax.rem(3 * wpad - 6 + 128, 128), 1)
                placed.append(jnp.where(lane128 < 3 * J, rolled, 0.0))
            for i in range(RB + 2):
                total = jnp.zeros((128, 128), jnp.float32)
                for dy in range(3):
                    ro = i - dy
                    if 0 <= ro < RB:
                        total = total + (pltpu.roll(placed[dy], 3 * J * ro, 1) if ro else placed[dy])
                wpo[i, c] = total.astype(jnp.bfloat16)
            return 0

        lax.fori_loop(0, J + 2, fill_out, 0)

        zc = jnp.zeros((R + 2, SUB, 256), jnp.bfloat16)
        act[:, J + 1] = zc

        sub16 = lax.broadcasted_iota(jnp.int32, (SUB, 128), 0)

        def scales(l, g):
            nh = 2 if l == 0 else 1
            per = 8 if l == 0 else 4
            for c in stat_copies(l, g):
                c.wait()
            for half in range(nh):
                x = stat_own[l % 2, g, half]
                for d in range(7):
                    x = x + stat_in[l % 2, g, d, half]
                k = 1
                while k < per:
                    x = x + jnp.where((lane8 & k) == 0, pltpu.roll(x, 128 - k, 1), pltpu.roll(x, k, 1))
                    k *= 2
                flip = pltpu.roll(x, 4, 0)
                mean = jnp.where(sub8 < 4, x, flip) / (count * per)
                var = jnp.where(sub8 < 4, flip, x) / (count * per) - mean * mean
                gain = nrm_ref[2 * l:2 * l + 1, half * 128:(half + 1) * 128]
                shift = nrm_ref[2 * l + 1:2 * l + 2, half * 128:(half + 1) * 128]
                s = lax.rsqrt(var + GN_EPS) * gain
                b = shift - mean * s
                sb[0, half] = 0.5 * jnp.concatenate([s, s], axis=0)
                sb[1, half] = 0.5 * jnp.concatenate([b, b], axis=0)

        def silu(x, half):
            u = x * sb[0, half] + sb[1, half]
            return u + u * jnp.tanh(u)

        def activate(l, g):
            nh = 2 if l == 0 else 1
            x = xbuf(l)

            def row(r, _):
                for j in range(J):
                    for half in range(nh):
                        sl = slice(half * 128, half * 128 + 128)
                        act[r + 1, j + 1, :, sl] = silu(x[g, r, j, :, sl].astype(jnp.float32), half).astype(jnp.bfloat16)
                return 0

            lax.fori_loop(0, R, row, 0)
            for c in halo_copies(l, g):
                c.wait()
            if l == 0:
                col, rw, cor = cola.at[g], rowa.at[g], cora.at[g]
            else:
                col, rw, cor = colx.at[l % 2, g], rowx.at[l % 2, g], corx.at[l % 2, g]

            def colrow(q, _):
                for k in range(8):
                    r = q * 8 + k
                    for half in range(nh):
                        sl = slice(half * 128, half * 128 + 128)
                        act[r + 1, 0, :, sl] = silu(col[r, :, sl].astype(jnp.float32), half).astype(jnp.bfloat16)
                return 0

            lax.fori_loop(0, R // 8, colrow, 0)
            for side in range(2):
                shift = NS if side == 0 else SUB - NS
                outer = (sub16 < NS) if side == 0 else (sub16 >= SUB - NS)
                border = jnp.logical_and(outer, sy == (0 if side == 0 else 3))
                own_row = R - 1 if side == 0 else 0
                for j in range(-1, J):
                    for half in range(nh):
                        sl = slice(half * 128, half * 128 + 128)
                        if j < 0:
                            own, far = col[own_row, :, sl], cor[side, :, sl]
                        else:
                            own, far = x[g, own_row, j, :, sl], rw[side, j, :, sl]
                        own = pltpu.roll(own.astype(jnp.float32), shift, 0)
                        far = pltpu.roll(far.astype(jnp.float32), shift, 0)
                        v = silu(jnp.where(outer, far, own), half)
                        v = jnp.where(border, 0.0, v)
                        act[0 if side == 0 else R + 1, j + 1, :, sl] = v.astype(jnp.bfloat16)

        def conv(l, g):
            ch = 256 if l == 0 else 128
            wp = wp1 if l == 0 else (wp2 if l == 1 else wpr.at[l - 2])
            out = xbuf(l + 1)
            if l == 1:
                bias = bias_ref[1:2] + bias_ref[6:7]
            else:
                bias = bias_ref[l:l + 1]
            bias = jnp.broadcast_to(bias.reshape(1, 1, 128), (BC, SUB, 128))

            def block(b, carry):
                one, two = carry
                r0 = b * BC
                rows = []
                for q in range(J // 2):
                    taps = []
                    for dy in range(3):
                        for d4 in range(4):
                            taps.append(act[pl.ds(r0 + dy, BC), 2 * q + d4, :, 0:ch].reshape(BC * SUB, ch))
                    if l == 1:
                        for s in range(2):
                            taps.append(a_buf[g, pl.ds(r0, BC), 2 * q + s].reshape(BC * SUB, 256))
                    rows.append(jnp.concatenate(taps, axis=1))
                lhs = jnp.concatenate(rows, axis=0)
                acc = jnp.dot(lhs, wp[...], preferred_element_type=jnp.float32)
                for q in range(J // 2):
                    for s in range(2):
                        v = acc[q * BC * SUB:(q + 1) * BC * SUB, s * 128:(s + 1) * 128].reshape(BC, SUB, 128) + bias
                        if l in (3, 5):
                            v = v + out[g, pl.ds(r0, BC), 2 * q + s].astype(jnp.float32)
                        v = v.astype(jnp.bfloat16)
                        out[g, pl.ds(r0, BC), 2 * q + s] = v
                        v = v.astype(jnp.float32)
                        one = one + jnp.sum(v, axis=0)
                        two = two + jnp.sum(v * v, axis=0)
                return one, two

            z = jnp.zeros((SUB, 128), jnp.float32)
            one, two = lax.fori_loop(0, R // BC, block, (z, z))
            sacc[0, 0] = one
            sacc[1, 0] = two

        def head(g):
            nb = R // RB
            taps = []
            for i in range(RB + 2):
                for c in range(J + 2):
                    parts = [act[RB * b + i, c, :, 0:128] for b in range(nb)]
                    taps.append(jnp.concatenate(parts, axis=0))
            acc = jnp.zeros((nb * SUB, 128), jnp.float32)
            for k in range(0, len(taps), 2):
                i, c = divmod(k, J + 2)
                w = wpo[i, pl.ds(c, 2)].reshape(256, 128)
                acc = acc + jnp.dot(jnp.concatenate(taps[k:k + 2], axis=1), w, preferred_element_type=jnp.float32)
            y_ref[g] = acc.reshape(nb, SUB, 128)

        for l in range(LAYERS):
            def phase(g, _, l=l):
                scales(l, g)
                activate(l, g)
                if l < LAYERS - 1:
                    conv(l, g)
                    push_stats(l + 1, g)
                    for c in halo_copies(l + 1, g):
                        c.start()
                else:
                    head(g)
                return 0

            lax.fori_loop(0, NG, phase, 0)

    def local_decode(act_in, norm_first, w_first, w_short, norm_rest, w_rest, bias_rest, w_out, bias_out):
        n, h, w, cin = act_in.shape
        rr = h // NG
        a = act_in.reshape(n, NG, rr, w, cin)
        f32 = jnp.float32
        nrm = jnp.concatenate([norm_first.astype(f32), jnp.pad(norm_rest.astype(f32).reshape(12, 128), ((0, 0), (0, 128)))], axis=0)
        nrm = jnp.pad(nrm, ((0, 2), (0, 0)))
        bias = jnp.pad(bias_rest.astype(f32), ((0, 1), (0, 0)))
        wo = jnp.transpose(w_out[:, ::-1], (0, 2, 1, 3)).reshape(3, 128, 9).astype(f32)
        wo = jnp.pad(wo, ((0, 0), (0, 0), (0, 119)))
        vm = pl.BlockSpec(memory_space=pltpu.VMEM)
        bf = jnp.bfloat16
        y = pl.pallas_call(
            kernel,
            out_shape=jax.ShapeDtypeStruct((NG, rr // RB, SUB, 128), f32),
            in_specs=[pl.BlockSpec(memory_space=pl.ANY)] + [vm] * 6,
            out_specs=vm,
            scratch_shapes=[
                pltpu.VMEM((NG, rr, J, SUB, 256), bf),
                pltpu.VMEM((NG, rr, J, SUB, 128), bf),
                pltpu.VMEM((NG, rr, J, SUB, 128), bf),
                pltpu.VMEM((NG, rr, SUB, 256), bf),
                pltpu.VMEM((2, NG, rr, SUB, 128), bf),
                pltpu.VMEM((NG, 2, J, SUB, 256), bf),
                pltpu.VMEM((2, NG, 2, J, SUB, 128), bf),
                pltpu.VMEM((NG, 2, SUB, 256), bf),
                pltpu.VMEM((2, NG, 2, SUB, 128), bf),
                pltpu.VMEM((rr + 2, J + 2, SUB, 256), bf),
                pltpu.VMEM((3072, 256), bf),
                pltpu.VMEM((2048, 256), bf),
                pltpu.VMEM((4, 1536, 256), bf),
                pltpu.VMEM((RB + 2, J + 2, 128, 128), bf),
                pltpu.VMEM((2, NS, NG, RC, J, 256), bf),
                pltpu.VMEM((2, 2, SUB * J, 128), f32),
                pltpu.VMEM((2, 2, SUB, 128), f32),
                pltpu.VMEM((2, NG, 2, 8, 128), f32),
                pltpu.VMEM((2, NG, 7, 2, 8, 128), f32),
                pltpu.VMEM((2, 2, SUB, 128), f32),
                pltpu.SemaphoreType.DMA((2,)),
                pltpu.SemaphoreType.DMA((LAYERS, NG)),
                pltpu.SemaphoreType.DMA((LAYERS, NG)),
                pltpu.SemaphoreType.DMA((LAYERS, NG, 2)),
                pltpu.SemaphoreType.DMA((LAYERS, NG, 2)),
                pltpu.SemaphoreType.DMA((LAYERS, NG, 2)),
                pltpu.SemaphoreType.DMA((LAYERS, NG, 2)),
                pltpu.SemaphoreType.DMA((LAYERS, NG, 7)),
                pltpu.SemaphoreType.DMA((LAYERS, NG, 7)),
            ],
            compiler_params=pltpu.CompilerParams(collective_id=0, has_side_effects=True, vmem_limit_bytes=67043328),
            name="decode",
        )(a, w_first, w_rest, w_short, wo, nrm, bias)
        y = y[..., :RB * J * 3].reshape(NG, rr // RB, NG, NS, RB, J, 3)
        y = jnp.transpose(y, (0, 3, 2, 1, 4, 5, 6)).reshape(n, h, w, 3)
        return y + bias_out.astype(f32)

    return jax.shard_map(local_decode, mesh=mesh, in_specs=(tile_spec,) + (rep,) * 8, out_specs=tile_spec, check_vma=False)
```

```python
import jax
import jax.numpy as jnp
from jax import lax
from jax.experimental import pallas as pl
from jax.experimental.pallas import tpu as pltpu
from jax.sharding import PartitionSpec as P

MESH = pl.DeviceIdType.MESH
GN_EPS = 1e-6
NG = 4
NS = 4
SUB = 16
J = 8
BC = 8
RC = 8
RB = 4
LAYERS = 7
CH = 128
CIN = 256
TAPS = 12


def solution(mesh):
    tile_spec = P("dp", "sy", "sx", None)
    rep = P()

    def kernel(a_hbm, w1_ref, wr_ref, ws_ref, wo_ref, n0_ref, nr_ref, bias_ref, bo_ref, y_ref,
               a_buf, t_buf, h_buf, rowa, rowx, cora, corx, act0, act1, act, wp1, wp2, wpr, wpo,
               raw, tmp, bias_rows, sacc, st_own, st_in, st_sum, st_far, sb,
               raw_sem, col_s, col_r, row_s, row_r, cor_s, cor_r, st_s, st_r, far_s, far_r):
        sx = lax.axis_index("sx")
        sy = lax.axis_index("sy")
        px = 1 - sx
        up = lax.rem(sy + 3, 4)
        dn = lax.rem(sy + 1, 4)
        R = a_buf.shape[1] - 2
        count = 1024.0 * 16.0
        f32, bf = jnp.float32, jnp.bfloat16

        barrier = pltpu.get_barrier_semaphore()
        friends = [{"sx": sx, "sy": lax.rem(sy + d, 4)} for d in range(1, 4)]
        friends += [{"sx": px, "sy": sy}, {"sx": px, "sy": up}, {"sx": px, "sy": dn}]
        for dev in friends:
            pl.semaphore_signal(barrier, inc=1, device_id=dev, device_id_type=MESH)

        def raw_copy(g, chunk, slot):
            return pltpu.make_async_copy(
                a_hbm.at[pl.ds(g * NS, NS), :, pl.ds(chunk * RC, RC)], raw.at[slot], raw_sem.at[slot])

        nchunk = R // RC
        raw_copy(0, 0, 0).start()

        def rcopy(src, dst, ss, rs, dev):
            return pltpu.make_async_remote_copy(src_ref=src, dst_ref=dst, send_sem=ss, recv_sem=rs, device_id=dev, device_id_type=MESH)

        def kind(l):
            return l if isinstance(l, int) else l[0]

        def index(l):
            return l if isinstance(l, int) else l[1]

        def after(l):
            return l + 1 if isinstance(l, int) else (5 - l[0], l[1] + 1)

        def halves(l):
            return 2 if kind(l) == 0 else 1

        def xbuf(l):
            return a_buf if kind(l) == 0 else (t_buf if kind(l) % 2 else h_buf)

        def halo_bufs(l, g):
            if kind(l) == 0:
                return rowa.at[g], cora.at[g]
            return rowx.at[kind(l) % 2, g], corx.at[kind(l) % 2, g]

        def halo_copies(l, g):
            x = xbuf(l)
            row, cor = halo_bufs(l, g)
            return [
                rcopy(x.at[g, R, pl.ds(1, J)], row.at[0], row_s.at[index(l), g, 0], row_r.at[index(l), g, 0], {"sx": sx, "sy": dn}),
                rcopy(x.at[g, 1, pl.ds(1, J)], row.at[1], row_s.at[index(l), g, 1], row_r.at[index(l), g, 1], {"sx": sx, "sy": up}),
                rcopy(x.at[g, R, 1], cor.at[0], cor_s.at[index(l), g, 0], cor_r.at[index(l), g, 0], {"sx": px, "sy": dn}),
                rcopy(x.at[g, 1, 1], cor.at[1], cor_s.at[index(l), g, 1], cor_r.at[index(l), g, 1], {"sx": px, "sy": up}),
                rcopy(x.at[g, pl.ds(1, R), 1], x.at[g, pl.ds(1, R), 0], col_s.at[index(l), g], col_r.at[index(l), g], {"sx": px, "sy": sy}),
            ]

        def near_copies(l, g):
            nh = halves(l)
            return [
                rcopy(st_own.at[kind(l) % 2, g, pl.ds(0, nh)], st_in.at[kind(l) % 2, g, d - 1, pl.ds(0, nh)],
                      st_s.at[index(l), g, d - 1], st_r.at[index(l), g, d - 1], friends[d - 1])
                for d in range(1, 4)
            ]

        def far_copy(l, g):
            nh = halves(l)
            return rcopy(st_sum.at[kind(l) % 2, g, pl.ds(0, nh)], st_far.at[kind(l) % 2, g, pl.ds(0, nh)],
                         far_s.at[index(l), g], far_r.at[index(l), g], {"sx": px, "sy": sy})

        sub8 = lax.broadcasted_iota(jnp.int32, (8, CH), 0)
        lane8 = lax.broadcasted_iota(jnp.int32, (8, CH), 1)
        sub16 = lax.broadcasted_iota(jnp.int32, (SUB, CH), 0)

        def fold(v):
            v = v[0:8] + v[8:16]
            return v + pltpu.roll(v, 4, 0)

        def push_sums(l, g):
            for half in range(halves(l)):
                st_own[kind(l) % 2, g, half] = jnp.where(sub8 < 4, fold(sacc[0, half]), fold(sacc[1, half]))
            for c in near_copies(l, g):
                c.start()

        def relay_sums(l, g):
            for c in near_copies(l, g):
                c.wait()
            for half in range(halves(l)):
                x = st_own[kind(l) % 2, g, half]
                for d in range(3):
                    x = x + st_in[kind(l) % 2, g, d, half]
                st_sum[kind(l) % 2, g, half] = x
            far_copy(l, g).start()

        def load_group(g, _):
            sacc[...] = jnp.zeros_like(sacc)

            def load_chunk(ch, _):
                step = g * nchunk + ch
                slot = lax.rem(step, 2)
                nxt = step + 1

                @pl.when(nxt < NG * nchunk)
                def _():
                    raw_copy(lax.div(nxt, nchunk), lax.rem(nxt, nchunk), lax.rem(nxt, 2)).start()

                raw_copy(g, ch, slot).wait()
                ones = [jnp.zeros((SUB, CH), f32) for _ in range(2)]
                twos = [jnp.zeros((SUB, CH), f32) for _ in range(2)]
                for r in range(RC):
                    for p in range(NG):
                        for i in range(NS):
                            v = raw[slot, i, p, r].astype(f32)
                            base = (p * NS + i) * J
                            tmp[r % 2, 0, base:base + J, :] = v[:, :CH]
                            tmp[r % 2, 1, base:base + J, :] = v[:, CH:]
                    for w in range(J):
                        j = sx * w + (1 - sx) * (J - 1 - w)
                        for half in range(2):
                            v = tmp[r % 2, half, pl.ds(w, SUB, stride=J), :]
                            a_buf[g, ch * RC + r + 1, j + 1, half] = v.astype(bf)
                            ones[half] = ones[half] + v
                            twos[half] = twos[half] + v * v
                for half in range(2):
                    sacc[0, half] = sacc[0, half] + ones[half]
                    sacc[1, half] = sacc[1, half] + twos[half]
                return 0

            lax.fori_loop(0, nchunk, load_chunk, 0)

            @pl.when(g == 0)
            def _():
                pl.semaphore_wait(barrier, len(friends))

            push_sums(0, g)

            @pl.when(g > 0)
            def _():
                relay_sums(0, g - 1)

            for c in halo_copies(0, g):
                c.start()
            return 0

        lax.fori_loop(0, NG, load_group, 0)

        def fill_pairs(dst, get, ch):
            zero = jnp.zeros((ch, CH), bf)
            for dy in range(3):
                for d4 in range(4):
                    k = (dy * 4 + d4) * ch
                    dst[k:k + ch, 0:CH] = get(dy, d4) if d4 < 3 else zero
                    dst[k:k + ch, CH:CIN] = get(dy, d4 - 1) if d4 > 0 else zero

        def real_dx(dx):
            return sx * dx + (1 - sx) * (2 - dx)

        fill_pairs(wp1, lambda dy, dx: w1_ref[dy, real_dx(dx)], CIN)
        relay_sums(0, NG - 1)
        fill_pairs(wp2, lambda dy, dx: wr_ref[0, dy, real_dx(dx)], CH)
        zs = jnp.zeros((CIN, CH), bf)
        wp2[1536:1792, 0:CH] = ws_ref[...]
        wp2[1536:1792, CH:CIN] = zs
        wp2[1792:2048, 0:CH] = zs
        wp2[1792:2048, CH:CIN] = ws_ref[...]

        def fill_rest(k, _):
            fill_pairs(wpr.at[k - 1], lambda dy, dx: wr_ref[k, dy, real_dx(dx)], CH)
            return 0

        lax.fori_loop(1, 5, fill_rest, 0)

        lane128 = lax.broadcasted_iota(jnp.int32, (CH, CH), 1)

        def fill_out(c, _):
            first = sx * c + (1 - sx) * (J + 1 - c) - 2
            tap = lax.rem(lane128, J) - first
            keep = (lane128 < 3 * J) & (tap >= 0) & (tap <= 2)
            placed = []
            for dy in range(3):
                placed.append(jnp.where(keep, pltpu.roll(wo_ref[dy], lax.rem(first + CH, CH), 1), 0.0))
            for i in range(RB + 2):
                total = jnp.zeros((CH, CH), f32)
                for dy in range(3):
                    ro = i - dy
                    if 0 <= ro < RB:
                        total = total + (pltpu.roll(placed[dy], 3 * J * ro, 1) if ro else placed[dy])
                k = pl.multiple_of((i * (J + 2) + c) * CH, CH)
                wpo[pl.ds(k, CH), :] = total.astype(bf)
            return 0

        lax.fori_loop(0, J + 2, fill_out, 0)

        act0[:, J + 1] = jnp.zeros((BC + 2, 2, SUB, CH), bf)
        act1[:, J + 1] = jnp.zeros((BC + 2, 2, SUB, CH), bf)
        act[:, J + 1] = jnp.zeros((R + 2, SUB, CH), bf)

        def scales(l, g):
            per = 8 if kind(l) == 0 else 4
            far_copy(l, g).wait()
            for half in range(halves(l)):
                x = st_sum[kind(l) % 2, g, half] + st_far[kind(l) % 2, g, half]
                k = 1
                while k < per:
                    x = x + jnp.where((lane8 & k) == 0, pltpu.roll(x, CH - k, 1), pltpu.roll(x, k, 1))
                    k *= 2
                flip = pltpu.roll(x, 4, 0)
                mean = jnp.where(sub8 < 4, x, flip) / (count * per)
                var = jnp.where(sub8 < 4, flip, x) / (count * per) - mean * mean
                if kind(l) == 0:
                    pair = n0_ref[:, half * CH:(half + 1) * CH].astype(f32)
                else:
                    pair = nr_ref[index(l) - 1].astype(f32)
                s = lax.rsqrt(var + GN_EPS) * pair[0:1]
                b = pair[1:2] - mean * s
                sb[0, half] = 0.5 * jnp.concatenate([s, s], axis=0)
                sb[1, half] = 0.5 * jnp.concatenate([b, b], axis=0)

        def finish_halo(l, g):
            x = xbuf(l)
            for c in halo_copies(l, g):
                c.wait()
            row, cor = halo_bufs(l, g)
            for side in range(2):
                shift = NS if side == 0 else SUB - NS
                outer = (sub16 < NS) if side == 0 else (sub16 >= SUB - NS)
                for j in range(J + 1):
                    for half in range(halves(l)):
                        own = x[g, R if side == 0 else 1, j, half].astype(f32)
                        far = (row[side, j - 1, half] if j else cor[side, half]).astype(f32)
                        v = jnp.where(outer, pltpu.roll(far, shift, 0), pltpu.roll(own, shift, 0))
                        x[g, 0 if side == 0 else R + 1, j, half] = v.astype(bf)

        def silu(x, half):
            u = x * sb[0, half] + sb[1, half]
            return u + u * jnp.tanh(u)

        top = (sub16 < NS) & (sy == 0)
        bottom = (sub16 >= SUB - NS) & (sy == 3)

        def activate(l, g, b, dst):
            x = xbuf(l)
            nb = R // BC
            for i in range(BC + 2):
                for half in range(halves(l)):
                    v = silu(x[g, b * BC + i, :, half].astype(f32), half)
                    if i == 0:
                        v = jnp.where(top & (b == 0), 0.0, v)
                    if i == BC + 1:
                        v = jnp.where(bottom & (b == nb - 1), 0.0, v)
                    dst[i, 0:J + 1, half] = v.astype(bf)

        def conv(l, g):
            wp = wp1 if kind(l) == 0 else (wp2 if kind(l) == 1 else wpr.at[index(l) - 2])
            out = xbuf(after(l))
            bias = bias_rows[pl.ds(index(l), 1), :]
            bias = jnp.broadcast_to(bias.reshape(1, 1, CH), (BC, SUB, CH))

            def block(b, src, one, two):
                r0 = b * BC
                rows = []
                for q in range(J // 2):
                    taps = []
                    for dy in range(3):
                        for d4 in range(4):
                            for half in range(halves(l)):
                                taps.append(src[dy:dy + BC, 2 * q + d4, half].reshape(BC * SUB, CH))
                    if kind(l) == 1:
                        for s in range(2):
                            for half in range(2):
                                taps.append(a_buf[g, pl.ds(r0 + 1, BC), 2 * q + s + 1, half].reshape(BC * SUB, CH))
                    rows.append(jnp.concatenate(taps, axis=1))
                lhs = jnp.concatenate(rows, axis=0)
                acc = jnp.dot(lhs, wp[...], preferred_element_type=f32)
                for q in range(J // 2):
                    for s in range(2):
                        at = (g, pl.ds(r0 + 1, BC), 2 * q + s + 1, 0)
                        v = acc[q * BC * SUB:(q + 1) * BC * SUB, s * CH:(s + 1) * CH].reshape(BC, SUB, CH) + bias
                        if kind(l) == 3:
                            v = v + out[at].astype(f32)
                        v = v.astype(bf)
                        out[at] = v
                        v = v.astype(f32)
                        one = one + jnp.sum(v, axis=0)
                        two = two + jnp.sum(v * v, axis=0)
                return one, two

            nb = R // BC
            activate(l, g, 0, act0)

            def step(i, carry):
                one, two = carry
                activate(l, g, 2 * i + 1, act1)
                one, two = block(2 * i, act0, one, two)
                activate(l, g, lax.rem(2 * i + 2, nb), act0)
                return block(2 * i + 1, act1, one, two)

            z = jnp.zeros((SUB, CH), f32)
            one, two = lax.fori_loop(0, nb // 2, step, (z, z))
            sacc[0, 0] = one
            sacc[1, 0] = two

        def head(g):
            x = h_buf
            nb = R // RB

            def row(r, _):
                for k in range(2):
                    act[2 * r + k, 0:J + 1] = silu(x[g, 2 * r + k, :, 0].astype(f32), 0).astype(bf)
                return 0

            lax.fori_loop(0, R // 2 + 1, row, 0)
            act[0, 0:J + 1] = jnp.where(top, 0.0, act[0, 0:J + 1].astype(f32)).astype(bf)
            act[R + 1, 0:J + 1] = jnp.where(bottom, 0.0, act[R + 1, 0:J + 1].astype(f32)).astype(bf)
            taps = []
            for i in range(RB + 2):
                for c in range(J + 2):
                    taps.append(jnp.concatenate([act[RB * b + i, c] for b in range(nb)], axis=0))
            acc = jnp.dot(jnp.concatenate(taps, axis=1), wpo[...], preferred_element_type=f32)
            acc = acc + bo_ref[...]
            for ro in range(RB):
                v = pltpu.roll(acc, CH - 3 * J * ro, 1) if ro else acc
                y_ref[g, :, ro] = v.reshape(nb, SUB, CH)

        biases = bias_ref[...].astype(f32)
        bias_rows[0:7] = biases
        bias_rows[1:2] = biases[1:2] + biases[6:7]

        def layer(l):
            def phase(g, _):
                if kind(l) > 0:
                    @pl.when(g == 1)
                    def _():
                        relay_sums(l, NG - 1)

                scales(l, g)
                finish_halo(l, g)
                if kind(l) == LAYERS - 1:
                    head(g)
                    return 0
                conv(l, g)
                push_sums(after(l), g)

                @pl.when(g > 0)
                def _():
                    relay_sums(after(l), g - 1)

                for c in halo_copies(after(l), g):
                    c.start()
                return 0

            lax.fori_loop(0, NG, phase, 0)

        layer(0)
        layer(1)

        def resnet(k, _):
            layer((2, 2 * k + 2))
            layer((3, 2 * k + 3))
            return 0

        lax.fori_loop(0, 2, resnet, 0)
        layer(6)

    def to_planes(x_ref, o_ref):
        rows = x_ref.shape[1] // SUB
        for i in range(NS):
            parts = [x_ref[0, pl.ds(p * NS + i, rows, stride=SUB), :] for p in range(NG)]
            flat = jnp.transpose(jnp.concatenate(parts, axis=0))
            o_ref[i] = flat[0:3 * J].reshape(3, J, NG * rows)

    def local_decode(act_in, norm_first, w_first, w_short, norm_rest, w_rest, bias_rest, w_out, bias_out):
        n, h, w, cin = act_in.shape
        rr = h // NG
        a = act_in.reshape(n, NG, rr, w, cin)
        f32 = jnp.float32
        lanes = jnp.arange(CH)[None, None, :]
        place = (lanes == (J * jnp.arange(3)[None, :, None] + 2 - jnp.arange(3)[:, None, None])).astype(jnp.bfloat16)
        wo = jnp.einsum("yxco,xol->ycl", w_out, place, preferred_element_type=f32)
        bo = jnp.tile(jnp.pad(jnp.repeat(bias_out.astype(f32), J), (0, 0)), RB)
        bo = jnp.pad(bo, (0, CH - 3 * J * RB)).reshape(1, CH)
        vm = pl.BlockSpec(memory_space=pltpu.VMEM)
        bf = jnp.bfloat16
        dma = pltpu.SemaphoreType.DMA
        y = pl.pallas_call(
            kernel,
            out_shape=jax.ShapeDtypeStruct((NG, rr // RB, RB, SUB, CH), f32),
            in_specs=[pl.BlockSpec(memory_space=pl.ANY)] + [vm] * 8,
            out_specs=vm,
            scratch_shapes=[
                pltpu.VMEM((NG, rr + 2, J + 1, 2, SUB, CH), bf),
                pltpu.VMEM((NG, rr + 2, J + 1, 1, SUB, CH), bf),
                pltpu.VMEM((NG, rr + 2, J + 1, 1, SUB, CH), bf),
                pltpu.VMEM((NG, 2, J, 2, SUB, CH), bf),
                pltpu.VMEM((2, NG, 2, J, 1, SUB, CH), bf),
                pltpu.VMEM((NG, 2, 2, SUB, CH), bf),
                pltpu.VMEM((2, NG, 2, 1, SUB, CH), bf),
                pltpu.VMEM((BC + 2, J + 2, 2, SUB, CH), bf),
                pltpu.VMEM((BC + 2, J + 2, 2, SUB, CH), bf),
                pltpu.VMEM((rr + 2, J + 2, SUB, CH), bf),
                pltpu.VMEM((TAPS * CIN, CIN), bf),
                pltpu.VMEM((2048, CIN), bf),
                pltpu.VMEM((NG, TAPS * CH, CIN), bf),
                pltpu.VMEM(((RB + 2) * (J + 2) * CH, CH), bf),
                pltpu.VMEM((2, NS, NG, RC, J, CIN), bf),
                pltpu.VMEM((2, 2, SUB * J, CH), f32),
                pltpu.VMEM((8, CH), f32),
                pltpu.VMEM((2, 2, SUB, CH), f32),
                pltpu.VMEM((2, NG, 2, 8, CH), f32),
                pltpu.VMEM((2, NG, 3, 2, 8, CH), f32),
                pltpu.VMEM((2, NG, 2, 8, CH), f32),
                pltpu.VMEM((2, NG, 2, 8, CH), f32),
                pltpu.VMEM((2, 2, SUB, CH), f32),
                dma((2,)),
                dma((LAYERS, NG)), dma((LAYERS, NG)),
                dma((LAYERS, NG, 2)), dma((LAYERS, NG, 2)),
                dma((LAYERS, NG, 2)), dma((LAYERS, NG, 2)),
                dma((LAYERS, NG, 3)), dma((LAYERS, NG, 3)),
                dma((LAYERS, NG)), dma((LAYERS, NG)),
            ],
            compiler_params=pltpu.CompilerParams(collective_id=0, has_side_effects=True, vmem_limit_bytes=67043328),
            name="decode",
        )(a, w_first, w_rest, w_short, wo, norm_first, norm_rest, bias_rest, bo)
        y = y.reshape(NG, rr * SUB, CH)
        y = pl.pallas_call(
            to_planes,
            grid=(NG,),
            out_shape=jax.ShapeDtypeStruct((n, 3, J, h), f32),
            in_specs=[pl.BlockSpec((1, rr * SUB, CH), lambda g: (g, 0, 0))],
            out_specs=pl.BlockSpec((NS, 3, J, h), lambda g: (g, 0, 0, 0)),
            name="to_planes",
        )(y)
        return jnp.transpose(y, (0, 3, 2, 1))

    return jax.shard_map(local_decode, mesh=mesh, in_specs=(tile_spec,) + (rep,) * 8, out_specs=tile_spec, check_vma=False)
```

```python
import jax
import jax.numpy as jnp
from jax import lax
from jax.experimental import pallas as pl
from jax.experimental.pallas import tpu as pltpu
from jax.sharding import PartitionSpec as P

MESH = pl.DeviceIdType.MESH
GN_EPS = 1e-6
NG = 4
NS = 4
SUB = 16
J = 8
BC = 16
RC = 8
RB = 4
HR = 6
LAYERS = 7
CH = 128
CIN = 256
TAPS = 14


def solution(mesh):
    tile_spec = P("dp", "sy", "sx", None)
    rep = P()

    def kernel(a_hbm, w1_ref, wr_ref, ws_ref, wo_ref, n0_ref, nr_ref, bias_ref, y_ref,
               a_buf, t_buf, h_buf, rowa, rowx, cora, corx, act0, act1, wp1, wp2, wpr, wpo,
               raw, tmp, ps_out, ps_in, bias_rows, sacc, st_own, st_in, st_sum, st_far, sb,
               raw_sem, col_s, col_r, row_s, row_r, cor_s, cor_r, st_s, st_r, far_s, far_r, ps_s, ps_r, pc_s, pc_r):
        sx = lax.axis_index("sx")
        sy = lax.axis_index("sy")
        px = 1 - sx
        up = lax.rem(sy + 3, 4)
        dn = lax.rem(sy + 1, 4)
        R = a_buf.shape[1] - 2
        count = 1024.0 * 16.0
        f32, bf = jnp.float32, jnp.bfloat16

        barrier = pltpu.get_barrier_semaphore()
        friends = [{"sx": sx, "sy": lax.rem(sy + d, 4)} for d in range(1, 4)]
        friends += [{"sx": px, "sy": sy}, {"sx": px, "sy": up}, {"sx": px, "sy": dn}]
        for dev in friends:
            pl.semaphore_signal(barrier, inc=1, device_id=dev, device_id_type=MESH)

        def raw_copy(g, chunk, slot):
            return pltpu.make_async_copy(
                a_hbm.at[pl.ds(g * NS, NS), :, pl.ds(chunk * RC, RC)], raw.at[slot], raw_sem.at[slot])

        nchunk = R // RC
        raw_copy(0, 0, 0).start()

        def rcopy(src, dst, ss, rs, dev):
            return pltpu.make_async_remote_copy(src_ref=src, dst_ref=dst, send_sem=ss, recv_sem=rs, device_id=dev, device_id_type=MESH)

        def kind(l):
            return l if isinstance(l, int) else l[0]

        def index(l):
            return l if isinstance(l, int) else l[1]

        def after(l):
            return l + 1 if isinstance(l, int) else (5 - l[0], l[1] + 1)

        def halves(l):
            return 2 if kind(l) == 0 else 1

        def xbuf(l):
            return a_buf if kind(l) == 0 else (t_buf if kind(l) % 2 else h_buf)

        def halo_bufs(l, g):
            if kind(l) == 0:
                return rowa.at[g], cora.at[g]
            return rowx.at[kind(l) % 2, g], corx.at[kind(l) % 2, g]

        def row_copies(l, g):
            x = xbuf(l)
            row, _ = halo_bufs(l, g)
            return [
                rcopy(x.at[g, R, pl.ds(1, J)], row.at[0], row_s.at[index(l), g, 0], row_r.at[index(l), g, 0], {"sx": sx, "sy": dn}),
                rcopy(x.at[g, 1, pl.ds(1, J)], row.at[1], row_s.at[index(l), g, 1], row_r.at[index(l), g, 1], {"sx": sx, "sy": up}),
            ]

        def piece_copy(ch):
            rows = pl.ds(ch * RC + 1, RC)
            return rcopy(a_buf.at[0, rows, 1], a_buf.at[0, rows, 0], pc_s.at[ch], pc_r.at[ch], {"sx": px, "sy": sy})

        def col_copy(l, g):
            x = xbuf(l)
            return rcopy(x.at[g, pl.ds(1, R), 1], x.at[g, pl.ds(1, R), 0], col_s.at[index(l), g], col_r.at[index(l), g], {"sx": px, "sy": sy})

        def corner_copies(l, g):
            x = xbuf(l)
            _, cor = halo_bufs(l, g)
            return [
                rcopy(x.at[g, R, 1], cor.at[0], cor_s.at[index(l), g, 0], cor_r.at[index(l), g, 0], {"sx": px, "sy": dn}),
                rcopy(x.at[g, 1, 1], cor.at[1], cor_s.at[index(l), g, 1], cor_r.at[index(l), g, 1], {"sx": px, "sy": up}),
            ]

        def start_halo(l, g):
            for c in row_copies(l, g):
                c.start()
            if kind(l) == 2:
                @pl.when(index(l) < LAYERS - 1)
                def _():
                    for c in corner_copies(l, g) + [col_copy(l, g)]:
                        c.start()
            else:
                for c in corner_copies(l, g):
                    c.start()
                if kind(l) == 0:
                    @pl.when(g > 0)
                    def _():
                        col_copy(l, g).start()
                else:
                    col_copy(l, g).start()

        def near_copies(l, g):
            nh = halves(l)
            return [
                rcopy(st_own.at[kind(l) % 2, g, pl.ds(0, nh)], st_in.at[kind(l) % 2, g, d - 1, pl.ds(0, nh)],
                      st_s.at[index(l), g, d - 1], st_r.at[index(l), g, d - 1], friends[d - 1])
                for d in range(1, 4)
            ]

        def far_copy(l, g):
            nh = halves(l)
            return rcopy(st_sum.at[kind(l) % 2, g, pl.ds(0, nh)], st_far.at[kind(l) % 2, g, pl.ds(0, nh)],
                         far_s.at[index(l), g], far_r.at[index(l), g], {"sx": px, "sy": sy})

        sub8 = lax.broadcasted_iota(jnp.int32, (8, CH), 0)
        lane8 = lax.broadcasted_iota(jnp.int32, (8, CH), 1)
        sub16 = lax.broadcasted_iota(jnp.int32, (SUB, CH), 0)

        def fold(v):
            v = v[0:8] + v[8:16]
            return v + pltpu.roll(v, 4, 0)

        def push_sums(l, g):
            for half in range(halves(l)):
                st_own[kind(l) % 2, g, half] = jnp.where(sub8 < 4, fold(sacc[0, half]), fold(sacc[1, half]))
            for c in near_copies(l, g):
                c.start()

        def relay_sums(l, g):
            for c in near_copies(l, g):
                c.wait()
            for half in range(halves(l)):
                x = st_own[kind(l) % 2, g, half]
                for d in range(3):
                    x = x + st_in[kind(l) % 2, g, d, half]
                st_sum[kind(l) % 2, g, half] = x
            far_copy(l, g).start()

        def load_group(g, _):
            sacc[...] = jnp.zeros_like(sacc)

            def load_chunk(ch, _):
                step = g * nchunk + ch
                slot = lax.rem(step, 2)
                nxt = step + 1

                @pl.when(nxt < NG * nchunk)
                def _():
                    raw_copy(lax.div(nxt, nchunk), lax.rem(nxt, nchunk), lax.rem(nxt, 2)).start()

                raw_copy(g, ch, slot).wait()
                ones = [jnp.zeros((SUB, CH), f32) for _ in range(2)]
                twos = [jnp.zeros((SUB, CH), f32) for _ in range(2)]
                for r in range(RC):
                    for p in range(NG):
                        for i in range(NS):
                            v = raw[slot, i, p, r].astype(f32)
                            base = (p * NS + i) * J
                            tmp[r % 2, 0, base:base + J, :] = v[:, :CH]
                            tmp[r % 2, 1, base:base + J, :] = v[:, CH:]
                    for w in range(J):
                        j = sx * w + (1 - sx) * (J - 1 - w)
                        for half in range(2):
                            v = tmp[r % 2, half, pl.ds(w, SUB, stride=J), :]
                            a_buf[g, ch * RC + r + 1, j + 1, half] = v.astype(bf)
                            ones[half] = ones[half] + v
                            twos[half] = twos[half] + v * v
                for half in range(2):
                    sacc[0, half] = sacc[0, half] + ones[half]
                    sacc[1, half] = sacc[1, half] + twos[half]

                @pl.when(g == 0)
                def _():
                    @pl.when(ch == 0)
                    def _():
                        pl.semaphore_wait(barrier, len(friends))

                    piece_copy(ch).start()

                return 0

            lax.fori_loop(0, nchunk, load_chunk, 0)

            push_sums(0, g)

            @pl.when(g > 0)
            def _():
                relay_sums(0, g - 1)

            start_halo(0, g)
            return 0

        lax.fori_loop(0, NG, load_group, 0)

        def fill_block(dst, w, ch, extra):
            zero = jnp.zeros((ch, CH), bf)

            def tap(dy, dx):
                return w[dy, sx * dx + (1 - sx) * (2 - dx)]

            parts = [(tap(0, 0), zero), (zero, tap(0, 2))]
            for dy in range(3):
                parts += [(tap(dy, 1), tap(dy, 0)), (tap(dy, 2), tap(dy, 1))]
            tail = [(tap(2, 0), zero), (zero, tap(2, 2))]
            for dx in (0, 2):
                tail += [(tap(1, dx), tap(0, dx)), (tap(2, dx), tap(1, dx))]
            k = 0
            for group in (parts, extra, tail):
                for left, right in group:
                    size = left.shape[0]
                    dst[k:k + size, 0:CH] = left
                    dst[k:k + size, CH:CIN] = right
                    k += size

        fill_block(wp1, w1_ref, CIN, [])
        relay_sums(0, NG - 1)
        fill_block(wp2, wr_ref.at[0], CH, [(ws_ref[...], jnp.zeros((CIN, CH), bf)), (jnp.zeros((CIN, CH), bf), ws_ref[...])])

        def fill_rest(k, _):
            fill_block(wpr.at[k - 1], wr_ref.at[k], CH, [])
            return 0

        lax.fori_loop(1, 5, fill_rest, 0)

        lane128 = lax.broadcasted_iota(jnp.int32, (CH, CH), 1)

        def place_rows(c, placed, col):
            for i in range(RB + 2):
                total = jnp.zeros((CH, CH), f32)
                for dy in range(3):
                    ro = i - dy
                    if 0 <= ro < RB:
                        total = total + (pltpu.roll(placed[dy], 3 * J * ro, 1) if ro else placed[dy])
                k = pl.multiple_of((i * J + c) * CH, CH)
                wpo[pl.ds(k, CH), col:col + CH] = total.astype(bf)

        def fill_out(c, _):
            first = sx * (c + 1) + (1 - sx) * (J - c) - 2
            tap = lax.rem(lane128, J) - first
            keep = (lane128 < 3 * J) & (tap >= 0) & (tap <= 2)
            place_rows(c, [jnp.where(keep, pltpu.roll(wo_ref[dy], lax.rem(first + CH, CH), 1), 0.0) for dy in range(3)], 0)
            for i in range(RB + 2):
                k = pl.multiple_of((i * J + c) * CH, CH)
                wpo[pl.ds(k, CH), CH:CIN] = jnp.zeros((CH, CH), bf)
            return 0

        lax.fori_loop(0, J, fill_out, 0)
        edge = (J - 1) * (1 - sx)
        far_edge = (J - 1) * sx
        keep = (lane128 < 3 * J) & (lax.rem(lane128, J) == far_edge)
        place_rows(0, [jnp.where(keep, pltpu.roll(wo_ref[dy], lax.rem(far_edge - 2 * (1 - sx) + CH, CH), 1), 0.0) for dy in range(3)], CH)

        for block_map in (act0, act1):
            block_map[:, :, J + 1] = jnp.zeros((BC // 2 + 1, 2, 2, SUB, CH), bf)

        def scales(l, g):
            per = 8 if kind(l) == 0 else 4
            far_copy(l, g).wait()
            for half in range(halves(l)):
                x = st_sum[kind(l) % 2, g, half] + st_far[kind(l) % 2, g, half]
                k = 1
                while k < per:
                    x = x + jnp.where((lane8 & k) == 0, pltpu.roll(x, CH - k, 1), pltpu.roll(x, k, 1))
                    k *= 2
                flip = pltpu.roll(x, 4, 0)
                mean = jnp.where(sub8 < 4, x, flip) / (count * per)
                var = jnp.where(sub8 < 4, flip, x) / (count * per) - mean * mean
                if kind(l) == 0:
                    pair = n0_ref[:, half * CH:(half + 1) * CH].astype(f32)
                else:
                    pair = nr_ref[index(l) - 1].astype(f32)
                s = lax.rsqrt(var + GN_EPS) * pair[0:1]
                b = pair[1:2] - mean * s
                sb[0, half] = 0.5 * jnp.concatenate([s, s], axis=0)
                sb[1, half] = 0.5 * jnp.concatenate([b, b], axis=0)

        def finish_halo(l, g):
            x = xbuf(l)
            last = kind(l) == LAYERS - 1
            for c in row_copies(l, g):
                c.wait()
            if not last:
                for c in corner_copies(l, g):
                    c.wait()
            if kind(l) == 0:
                @pl.when(g == 0)
                def _():
                    for ch in range(nchunk):
                        piece_copy(ch).wait()

                @pl.when(g > 0)
                def _():
                    col_copy(l, g).wait()
            elif not last:
                col_copy(l, g).wait()
            row, cor = halo_bufs(l, g)
            for side in range(2):
                shift = NS if side == 0 else SUB - NS
                outer = (sub16 < NS) if side == 0 else (sub16 >= SUB - NS)
                for j in range(1 if last else 0, J + 1):
                    for half in range(halves(l)):
                        own = x[g, R if side == 0 else 1, j, half].astype(f32)
                        far = (row[side, j - 1, half] if j else cor[side, half]).astype(f32)
                        v = jnp.where(outer, pltpu.roll(far, shift, 0), pltpu.roll(own, shift, 0))
                        x[g, 0 if side == 0 else R + 1, j, half] = v.astype(bf)

        def silu(x, half):
            u = x * sb[0, half] + sb[1, half]
            return u + u * jnp.tanh(u)

        top = (sub16 < NS) & (sy == 0)
        bottom = (sub16 >= SUB - NS) & (sy == 3)

        def activate(l, g, b, dst):
            x = xbuf(l)
            nb = R // BC
            for i in range(BC + 2):
                for half in range(halves(l)):
                    v = silu(x[g, b * BC + i, :, half].astype(f32), half)
                    if i == 0:
                        v = jnp.where(top & (b == 0), 0.0, v)
                    if i == BC + 1:
                        v = jnp.where(bottom & (b == nb - 1), 0.0, v)
                    dst[i // 2, i % 2, 0:J + 1, half] = v.astype(bf)

        def conv(l, g):
            wp = wp1 if kind(l) == 0 else (wp2 if kind(l) == 1 else wpr.at[index(l) - 2])
            out = xbuf(after(l))
            bias = bias_rows[pl.ds(index(l), 1), :]
            bias = jnp.broadcast_to(bias.reshape(1, 1, CH), (BC, SUB, CH))

            half_rows = BC // 2
            ch = CH * halves(l)
            mid = 6 * ch + (2 * CIN if kind(l) == 1 else 0)

            def block(b, src, one, two):
                r0 = b * BC
                m = half_rows * SUB

                def pixel(t, col):
                    return [src[t // 2:t // 2 + half_rows, t % 2, col, half].reshape(m, CH) for half in range(halves(l))]

                def stack(columns):
                    return jnp.concatenate([jnp.concatenate(columns(2 * q), axis=1) for q in range(J // 2)], axis=0)

                skips = []
                if kind(l) == 1:
                    for c in range(J):
                        skips.append([a_buf[g, pl.ds(r0 + 1, BC), c + 1, half].reshape(half_rows, 2, SUB, CH) for half in range(2)])

                def taps(r, q2):
                    own = []
                    for dy in range(3):
                        own += pixel(r + dy, q2 + 1) + pixel(r + dy, q2 + 2)
                    if kind(l) == 1:
                        own += [v[:, r:r + 1].reshape(m, CH) for c in range(2) for v in skips[q2 + c]]
                    corner = pixel(3 * r, q2) + pixel(3 * r, q2 + 3)
                    return own + corner if r else corner + own

                def mm(lhs, start, size):
                    return jnp.dot(lhs, wp[start:start + size, :], preferred_element_type=f32)

                rows = [mm(stack(lambda q2: taps(r, q2)), 2 * ch * r, mid + 2 * ch) for r in range(2)]
                base = mid + 4 * ch
                sides = [mm(stack(lambda q2: pixel(1, q2 + 3 * s) + pixel(2, q2 + 3 * s)), base + 2 * ch * s, 2 * ch) for s in range(2)]
                for q in range(J // 2):
                    for s in range(2):
                        pair = []
                        for r in range(2):
                            v = rows[r][q * m:(q + 1) * m, s * CH:(s + 1) * CH] + sides[s][q * m:(q + 1) * m, r * CH:(r + 1) * CH]
                            pair.append(v.reshape(half_rows, 1, SUB, CH))
                        v = jnp.concatenate(pair, axis=1).reshape(BC, SUB, CH) + bias
                        at = (g, pl.ds(r0 + 1, BC), 2 * q + s + 1, 0)
                        if kind(l) == 3:
                            v = v + out[at].astype(f32)
                        v = v.astype(bf)
                        out[at] = v
                        v = v.astype(f32)
                        one = one + jnp.sum(v, axis=0)
                        two = two + jnp.sum(v * v, axis=0)
                return one, two

            nb = R // BC
            activate(l, g, 0, act0)

            def step(i, carry):
                one, two = carry
                activate(l, g, 2 * i + 1, act1)
                one, two = block(2 * i, act0, one, two)
                activate(l, g, lax.rem(2 * i + 2, nb), act0)
                return block(2 * i + 1, act1, one, two)

            z = jnp.zeros((SUB, CH), f32)
            one, two = lax.fori_loop(0, nb // 2, step, (z, z))
            sacc[0, 0] = one
            sacc[1, 0] = two

        nblk = R // RB

        def edge_copy(g):
            return rcopy(ps_out.at[g], ps_in.at[g], ps_s.at[g], ps_r.at[g], {"sx": px, "sy": sy})

        def head_act(g):
            def rows(step, _):
                for k in range(HR):
                    r = HR * step + k
                    t_buf[g, r, 0:J, 0] = silu(h_buf[g, r, 1:J + 1, 0].astype(f32), 0).astype(bf)
                return 0

            lax.fori_loop(0, (R + 2) // HR, rows, 0)
            for r, border in ((0, top), (R + 1, bottom)):
                t_buf[g, r, 0:J, 0] = jnp.where(border, 0.0, t_buf[g, r, 0:J, 0].astype(f32)).astype(bf)

        def head(g):
            taps = []
            for i in range(RB + 2):
                for c in range(J):
                    taps.append(jnp.concatenate([t_buf[g, RB * b + i, c, 0] for b in range(nblk)], axis=0))
            acc = jnp.dot(jnp.concatenate(taps, axis=1), wpo[...], preferred_element_type=f32)
            y_ref[g] = acc[:, 0:CH].reshape(nblk, SUB, CH)
            for part in range(nblk // J):
                total = jnp.zeros((SUB, CH), f32)
                for k in range(J):
                    b = part * J + k
                    total = total + pltpu.roll(acc[b * SUB:(b + 1) * SUB, CH:CIN], lax.rem(k - far_edge + CH, CH), 1)
                ps_out[g, part] = total
            edge_copy(g).start()

        def add_edges(g, _):
            edge_copy(g).wait()
            lane16 = lax.broadcasted_iota(jnp.int32, (SUB, CH), 1)
            mine = (lane16 < 3 * J * RB) & (lax.rem(lane16, J) == edge)
            for b in range(nblk):
                v = pltpu.roll(ps_in[g, b // J], lax.rem(edge - b % J + CH, CH), 1)
                y_ref[g, b] = y_ref[g, b] + jnp.where(mine, v, 0.0)
            return 0

        biases = bias_ref[...].astype(f32)
        bias_rows[0:7] = biases
        bias_rows[1:2] = biases[1:2] + biases[6:7]

        def layer(l):
            def phase(g, _):
                if kind(l) > 0:
                    @pl.when(g == 1)
                    def _():
                        relay_sums(l, NG - 1)

                scales(l, g)
                finish_halo(l, g)
                conv(l, g)
                push_sums(after(l), g)

                @pl.when(g > 0)
                def _():
                    relay_sums(after(l), g - 1)

                start_halo(after(l), g)
                return 0

            lax.fori_loop(0, NG, phase, 0)

        layer(0)
        layer(1)

        def resnet(k, _):
            layer((2, 2 * k + 2))
            layer((3, 2 * k + 3))
            return 0

        lax.fori_loop(0, 2, resnet, 0)
        def last(g, _):
            @pl.when(g == 1)
            def _():
                relay_sums(LAYERS - 1, NG - 1)

            scales(LAYERS - 1, g)
            finish_halo(LAYERS - 1, g)
            head_act(g)
            head(g)
            return 0

        lax.fori_loop(0, NG, last, 0)
        lax.fori_loop(0, NG, add_edges, 0)

    def to_planes(x_ref, b_ref, o_ref, ys):
        bias = b_ref[...].astype(jnp.float32)
        blocks = x_ref.shape[1]
        rows = blocks * RB
        v = x_ref[0].reshape(blocks * SUB, CH)
        for ro in range(RB):
            u = pltpu.roll(v, CH - 3 * J * ro, 1) if ro else v
            for b in range(blocks):
                ys[(RB * b + ro) * SUB:(RB * b + ro + 1) * SUB] = u[b * SUB:(b + 1) * SUB]
        for i in range(NS):
            parts = [ys[pl.ds(p * NS + i, rows, stride=SUB), :] for p in range(NG)]
            flat = jnp.transpose(jnp.concatenate(parts, axis=0))
            for c in range(3):
                o_ref[i, c] = flat[c * J:(c + 1) * J] + bias[:, c:c + 1]

    def local_decode(act_in, norm_first, w_first, w_short, norm_rest, w_rest, bias_rest, w_out, bias_out):
        n, h, w, cin = act_in.shape
        rr = h // NG
        a = act_in.reshape(n, NG, rr, w, cin)
        f32 = jnp.float32
        lanes = jnp.arange(CH)[None, None, :]
        place = (lanes == (J * jnp.arange(3)[None, :, None] + 2 - jnp.arange(3)[:, None, None])).astype(jnp.bfloat16)
        wo = jnp.einsum("yxco,xol->ycl", w_out, place, preferred_element_type=f32)
        vm = pl.BlockSpec(memory_space=pltpu.VMEM)
        bf = jnp.bfloat16
        dma = pltpu.SemaphoreType.DMA
        block_map = pltpu.VMEM((BC // 2 + 1, 2, J + 2, 2, SUB, CH), bf)
        sides = dma((LAYERS, NG, 2))
        y = pl.pallas_call(
            kernel,
            out_shape=jax.ShapeDtypeStruct((NG, rr // RB, SUB, CH), f32),
            in_specs=[pl.BlockSpec(memory_space=pl.ANY)] + [vm] * 7,
            out_specs=vm,
            scratch_shapes=[
                pltpu.VMEM((NG, rr + 2, J + 1, 2, SUB, CH), bf),
                pltpu.VMEM((NG, rr + 2, J + 1, 1, SUB, CH), bf),
                pltpu.VMEM((NG, rr + 2, J + 1, 1, SUB, CH), bf),
                pltpu.VMEM((NG, 2, J, 2, SUB, CH), bf),
                pltpu.VMEM((2, NG, 2, J, 1, SUB, CH), bf),
                pltpu.VMEM((NG, 2, 2, SUB, CH), bf),
                pltpu.VMEM((2, NG, 2, 1, SUB, CH), bf),
                block_map, block_map,
                pltpu.VMEM((TAPS * CIN, CIN), bf),
                pltpu.VMEM((TAPS * CH + 2 * CIN, CIN), bf),
                pltpu.VMEM((NG, TAPS * CH, CIN), bf),
                pltpu.VMEM(((RB + 2) * J * CH, CIN), bf),
                pltpu.VMEM((2, NS, NG, RC, J, CIN), bf),
                pltpu.VMEM((2, 2, SUB * J, CH), f32),
                pltpu.VMEM((NG, rr // RB // J, SUB, CH), f32),
                pltpu.VMEM((NG, rr // RB // J, SUB, CH), f32),
                pltpu.VMEM((8, CH), f32),
                pltpu.VMEM((2, 2, SUB, CH), f32),
                pltpu.VMEM((2, NG, 2, 8, CH), f32),
                pltpu.VMEM((2, NG, 3, 2, 8, CH), f32),
                pltpu.VMEM((2, NG, 2, 8, CH), f32),
                pltpu.VMEM((2, NG, 2, 8, CH), f32),
                pltpu.VMEM((2, 2, SUB, CH), f32),
                dma((2,)),
                dma((LAYERS, NG)), dma((LAYERS, NG)),
                sides, sides, sides, sides,
                dma((LAYERS, NG, 3)), dma((LAYERS, NG, 3)),
                dma((LAYERS, NG)), dma((LAYERS, NG)),
                dma((NG,)), dma((NG,)),
                dma((rr // RC,)), dma((rr // RC,)),
            ],
            compiler_params=pltpu.CompilerParams(collective_id=0, has_side_effects=True, vmem_limit_bytes=67043328),
            name="decode",
        )(a, w_first, w_rest, w_short, wo, norm_first, norm_rest, bias_rest)
        y = pl.pallas_call(
            to_planes,
            grid=(NG,),
            out_shape=jax.ShapeDtypeStruct((n, 3, J, h), f32),
            in_specs=[pl.BlockSpec((1, rr // RB, SUB, CH), lambda g: (g, 0, 0, 0)), pl.BlockSpec((1, 3), lambda g: (0, 0))],
            out_specs=pl.BlockSpec((NS, 3, J, h), lambda g: (g, 0, 0, 0)),
            scratch_shapes=[pltpu.VMEM((rr * SUB, CH), f32)],
            name="to_planes",
        )(y, bias_out.reshape(1, 3))
        return jnp.transpose(y, (0, 3, 2, 1))

    return jax.shard_map(local_decode, mesh=mesh, in_specs=(tile_spec,) + (rep,) * 8, out_specs=tile_spec, check_vma=False)
```

```python
import jax
import jax.numpy as jnp
from jax import lax
from jax.experimental import pallas as pl
from jax.experimental.pallas import tpu as pltpu
from jax.sharding import PartitionSpec as P

MESH = pl.DeviceIdType.MESH
GN_EPS = 1e-6
NG = 4
NS = 4
SUB = 16
J = 8
BC = 16
RC = 8
SLOTS = 4
RB = 4
HR = 6
LAYERS = 7
CH = 128
CIN = 256
TAPS = 14


def solution(mesh):
    tile_spec = P("dp", "sy", "sx", None)
    rep = P()

    def kernel(a_hbm, w1_ref, wr_ref, ws_ref, wo_ref, n0_ref, nr_ref, bias_ref, y_ref,
               a_buf, t_buf, h_buf, rowa, rowx, cora, corx, act0, act1, wp1, wp2, wpr, wpo,
               raw, tmp, ps_out, ps_in, bias_rows, sacc, st_own, st_in, st_sum, st_far, sb,
               raw_sem, col_s, col_r, row_s, row_r, cor_s, cor_r, st_s, st_r, far_s, far_r, ps_s, ps_r, pc_s, pc_r):
        sx = lax.axis_index("sx")
        sy = lax.axis_index("sy")
        px = 1 - sx
        up = lax.rem(sy + 3, 4)
        dn = lax.rem(sy + 1, 4)
        R = a_buf.shape[1] - 2
        count = 1024.0 * 16.0
        f32, bf = jnp.float32, jnp.bfloat16

        barrier = pltpu.get_barrier_semaphore()
        friends = [{"sx": sx, "sy": lax.rem(sy + d, 4)} for d in range(1, 4)]
        friends += [{"sx": px, "sy": sy}, {"sx": px, "sy": up}, {"sx": px, "sy": dn}]
        for dev in friends:
            pl.semaphore_signal(barrier, inc=1, device_id=dev, device_id_type=MESH)

        def raw_copy(g, chunk, slot):
            return pltpu.make_async_copy(
                a_hbm.at[pl.ds(g * NS, NS), :, pl.ds(chunk * RC, RC)], raw.at[slot], raw_sem.at[slot])

        nchunk = R // RC
        for ahead in range(SLOTS - 1):
            raw_copy(0, ahead, ahead).start()

        def rcopy(src, dst, ss, rs, dev):
            return pltpu.make_async_remote_copy(src_ref=src, dst_ref=dst, send_sem=ss, recv_sem=rs, device_id=dev, device_id_type=MESH)

        def kind(l):
            return l if isinstance(l, int) else l[0]

        def index(l):
            return l if isinstance(l, int) else l[1]

        def after(l):
            return l + 1 if isinstance(l, int) else (5 - l[0], l[1] + 1)

        def halves(l):
            return 2 if kind(l) == 0 else 1

        def xbuf(l):
            return a_buf if kind(l) == 0 else (t_buf if kind(l) % 2 else h_buf)

        def halo_bufs(l, g):
            if kind(l) == 0:
                return rowa.at[g], cora.at[g]
            return rowx.at[kind(l) % 2, g], corx.at[kind(l) % 2, g]

        def row_copies(l, g):
            x = xbuf(l)
            row, _ = halo_bufs(l, g)
            return [
                rcopy(x.at[g, R, pl.ds(1, J)], row.at[0], row_s.at[index(l), g, 0], row_r.at[index(l), g, 0], {"sx": sx, "sy": dn}),
                rcopy(x.at[g, 1, pl.ds(1, J)], row.at[1], row_s.at[index(l), g, 1], row_r.at[index(l), g, 1], {"sx": sx, "sy": up}),
            ]

        def piece_copy(ch):
            rows = pl.ds(ch * RC + 1, RC)
            return rcopy(a_buf.at[0, rows, 1], a_buf.at[0, rows, 0], pc_s.at[ch], pc_r.at[ch], {"sx": px, "sy": sy})

        def col_copy(l, g):
            x = xbuf(l)
            return rcopy(x.at[g, pl.ds(1, R), 1], x.at[g, pl.ds(1, R), 0], col_s.at[index(l), g], col_r.at[index(l), g], {"sx": px, "sy": sy})

        def corner_copies(l, g):
            x = xbuf(l)
            _, cor = halo_bufs(l, g)
            return [
                rcopy(x.at[g, R, 1], cor.at[0], cor_s.at[index(l), g, 0], cor_r.at[index(l), g, 0], {"sx": px, "sy": dn}),
                rcopy(x.at[g, 1, 1], cor.at[1], cor_s.at[index(l), g, 1], cor_r.at[index(l), g, 1], {"sx": px, "sy": up}),
            ]

        def start_halo(l, g):
            for c in row_copies(l, g):
                c.start()
            if kind(l) == 2:
                @pl.when(index(l) < LAYERS - 1)
                def _():
                    for c in corner_copies(l, g) + [col_copy(l, g)]:
                        c.start()
            else:
                for c in corner_copies(l, g):
                    c.start()
                if kind(l) == 0:
                    @pl.when(g > 0)
                    def _():
                        col_copy(l, g).start()
                else:
                    col_copy(l, g).start()

        def near_copies(l, g):
            nh = halves(l)
            return [
                rcopy(st_own.at[kind(l) % 2, g, pl.ds(0, nh)], st_in.at[kind(l) % 2, g, d - 1, pl.ds(0, nh)],
                      st_s.at[index(l), g, d - 1], st_r.at[index(l), g, d - 1], friends[d - 1])
                for d in range(1, 4)
            ]

        def far_copy(l, g):
            nh = halves(l)
            return rcopy(st_sum.at[kind(l) % 2, g, pl.ds(0, nh)], st_far.at[kind(l) % 2, g, pl.ds(0, nh)],
                         far_s.at[index(l), g], far_r.at[index(l), g], {"sx": px, "sy": sy})

        sub8 = lax.broadcasted_iota(jnp.int32, (8, CH), 0)
        lane8 = lax.broadcasted_iota(jnp.int32, (8, CH), 1)
        sub16 = lax.broadcasted_iota(jnp.int32, (SUB, CH), 0)

        def fold(v):
            v = v[0:8] + v[8:16]
            return v + pltpu.roll(v, 4, 0)

        def push_sums(l, g):
            for half in range(halves(l)):
                st_own[kind(l) % 2, g, half] = jnp.where(sub8 < 4, fold(sacc[0, half]), fold(sacc[1, half]))
            for c in near_copies(l, g):
                c.start()

        def relay_sums(l, g):
            for c in near_copies(l, g):
                c.wait()
            for half in range(halves(l)):
                x = st_own[kind(l) % 2, g, half]
                for d in range(3):
                    x = x + st_in[kind(l) % 2, g, d, half]
                st_sum[kind(l) % 2, g, half] = x
            far_copy(l, g).start()

        def load_group(g, _):
            sacc[...] = jnp.zeros_like(sacc)

            def load_chunk(ch, _):
                step = g * nchunk + ch
                slot = lax.rem(step, SLOTS)
                nxt = step + SLOTS - 1

                @pl.when(nxt < NG * nchunk)
                def _():
                    raw_copy(lax.div(nxt, nchunk), lax.rem(nxt, nchunk), lax.rem(nxt, SLOTS)).start()

                raw_copy(g, ch, slot).wait()
                ones = [jnp.zeros((SUB, CH), f32) for _ in range(2)]
                twos = [jnp.zeros((SUB, CH), f32) for _ in range(2)]
                for r in range(RC):
                    for p in range(NG):
                        for i in range(NS):
                            v = raw[slot, i, p, r].astype(f32)
                            base = (p * NS + i) * J
                            tmp[r % 2, 0, base:base + J, :] = v[:, :CH]
                            tmp[r % 2, 1, base:base + J, :] = v[:, CH:]
                    for w in range(J):
                        j = sx * w + (1 - sx) * (J - 1 - w)
                        for half in range(2):
                            v = tmp[r % 2, half, pl.ds(w, SUB, stride=J), :]
                            a_buf[g, ch * RC + r + 1, j + 1, half] = v.astype(bf)
                            ones[half] = ones[half] + v
                            twos[half] = twos[half] + v * v
                for half in range(2):
                    sacc[0, half] = sacc[0, half] + ones[half]
                    sacc[1, half] = sacc[1, half] + twos[half]

                @pl.when(g == 0)
                def _():
                    @pl.when(ch == 0)
                    def _():
                        pl.semaphore_wait(barrier, len(friends))

                    piece_copy(ch).start()

                return 0

            lax.fori_loop(0, nchunk, load_chunk, 0)

            push_sums(0, g)

            @pl.when(g > 0)
            def _():
                relay_sums(0, g - 1)

            start_halo(0, g)
            return 0

        lax.fori_loop(0, NG, load_group, 0)

        def fill_block(dst, w, ch, extra):
            zero = jnp.zeros((ch, CH), bf)

            def tap(dy, dx):
                return w[dy, sx * dx + (1 - sx) * (2 - dx)]

            parts = [(tap(0, 0), zero), (zero, tap(0, 2))]
            for dy in range(3):
                parts += [(tap(dy, 1), tap(dy, 0)), (tap(dy, 2), tap(dy, 1))]
            tail = [(tap(2, 0), zero), (zero, tap(2, 2))]
            for dx in (0, 2):
                tail += [(tap(1, dx), tap(0, dx)), (tap(2, dx), tap(1, dx))]
            k = 0
            for group in (parts, extra, tail):
                for left, right in group:
                    size = left.shape[0]
                    dst[k:k + size, 0:CH] = left
                    dst[k:k + size, CH:CIN] = right
                    k += size

        fill_block(wp1, w1_ref, CIN, [])
        relay_sums(0, NG - 1)
        fill_block(wp2, wr_ref.at[0], CH, [(ws_ref[...], jnp.zeros((CIN, CH), bf)), (jnp.zeros((CIN, CH), bf), ws_ref[...])])

        def fill_rest(k, _):
            fill_block(wpr.at[k - 1], wr_ref.at[k], CH, [])
            return 0

        lax.fori_loop(1, 5, fill_rest, 0)

        lane128 = lax.broadcasted_iota(jnp.int32, (CH, CH), 1)

        def place_rows(c, placed, col):
            for i in range(RB + 2):
                total = jnp.zeros((CH, CH), f32)
                for dy in range(3):
                    ro = i - dy
                    if 0 <= ro < RB:
                        total = total + (pltpu.roll(placed[dy], 3 * J * ro, 1) if ro else placed[dy])
                k = pl.multiple_of((i * J + c) * CH, CH)
                wpo[pl.ds(k, CH), col:col + CH] = total.astype(bf)

        def fill_out(c, _):
            first = sx * (c + 1) + (1 - sx) * (J - c) - 2
            tap = lax.rem(lane128, J) - first
            keep = (lane128 < 3 * J) & (tap >= 0) & (tap <= 2)
            place_rows(c, [jnp.where(keep, pltpu.roll(wo_ref[dy], lax.rem(first + CH, CH), 1), 0.0) for dy in range(3)], 0)
            for i in range(RB + 2):
                k = pl.multiple_of((i * J + c) * CH, CH)
                wpo[pl.ds(k, CH), CH:CIN] = jnp.zeros((CH, CH), bf)
            return 0

        lax.fori_loop(0, J, fill_out, 0)
        edge = (J - 1) * (1 - sx)
        far_edge = (J - 1) * sx
        keep = (lane128 < 3 * J) & (lax.rem(lane128, J) == far_edge)
        place_rows(0, [jnp.where(keep, pltpu.roll(wo_ref[dy], lax.rem(far_edge - 2 * (1 - sx) + CH, CH), 1), 0.0) for dy in range(3)], CH)

        for block_map in (act0, act1):
            block_map[:, :, J + 1] = jnp.zeros((BC // 2 + 1, 2, 2, SUB, CH), bf)

        def scales(l, g):
            per = 8 if kind(l) == 0 else 4
            far_copy(l, g).wait()
            for half in range(halves(l)):
                x = st_sum[kind(l) % 2, g, half] + st_far[kind(l) % 2, g, half]
                k = 1
                while k < per:
                    x = x + jnp.where((lane8 & k) == 0, pltpu.roll(x, CH - k, 1), pltpu.roll(x, k, 1))
                    k *= 2
                flip = pltpu.roll(x, 4, 0)
                mean = jnp.where(sub8 < 4, x, flip) / (count * per)
                var = jnp.where(sub8 < 4, flip, x) / (count * per) - mean * mean
                if kind(l) == 0:
                    pair = n0_ref[:, half * CH:(half + 1) * CH].astype(f32)
                else:
                    pair = nr_ref[index(l) - 1].astype(f32)
                s = lax.rsqrt(var + GN_EPS) * pair[0:1]
                b = pair[1:2] - mean * s
                sb[0, half] = 0.5 * jnp.concatenate([s, s], axis=0)
                sb[1, half] = 0.5 * jnp.concatenate([b, b], axis=0)

        def finish_halo(l, g):
            x = xbuf(l)
            last = kind(l) == LAYERS - 1
            for c in row_copies(l, g):
                c.wait()
            if not last:
                for c in corner_copies(l, g):
                    c.wait()
            if kind(l) == 0:
                @pl.when(g == 0)
                def _():
                    for ch in range(nchunk):
                        piece_copy(ch).wait()

                @pl.when(g > 0)
                def _():
                    col_copy(l, g).wait()
            elif not last:
                col_copy(l, g).wait()
            row, cor = halo_bufs(l, g)
            for side in range(2):
                shift = NS if side == 0 else SUB - NS
                outer = (sub16 < NS) if side == 0 else (sub16 >= SUB - NS)
                for j in range(1 if last else 0, J + 1):
                    for half in range(halves(l)):
                        own = x[g, R if side == 0 else 1, j, half].astype(f32)
                        far = (row[side, j - 1, half] if j else cor[side, half]).astype(f32)
                        v = jnp.where(outer, pltpu.roll(far, shift, 0), pltpu.roll(own, shift, 0))
                        x[g, 0 if side == 0 else R + 1, j, half] = v.astype(bf)

        def silu(x, half):
            u = x * sb[0, half] + sb[1, half]
            return u + u * jnp.tanh(u)

        top = (sub16 < NS) & (sy == 0)
        bottom = (sub16 >= SUB - NS) & (sy == 3)

        def activate(l, g, b, dst):
            x = xbuf(l)
            nb = R // BC
            for i in range(BC + 2):
                for half in range(halves(l)):
                    v = silu(x[g, b * BC + i, :, half].astype(f32), half)
                    if i == 0:
                        v = jnp.where(top & (b == 0), 0.0, v)
                    if i == BC + 1:
                        v = jnp.where(bottom & (b == nb - 1), 0.0, v)
                    dst[i // 2, i % 2, 0:J + 1, half] = v.astype(bf)

        def conv(l, g):
            wp = wp1 if kind(l) == 0 else (wp2 if kind(l) == 1 else wpr.at[index(l) - 2])
            out = xbuf(after(l))
            bias = bias_rows[pl.ds(index(l), 1), :]
            bias = jnp.broadcast_to(bias.reshape(1, 1, CH), (BC, SUB, CH))

            half_rows = BC // 2
            ch = CH * halves(l)
            mid = 6 * ch + (2 * CIN if kind(l) == 1 else 0)

            def block(b, src, one, two):
                r0 = b * BC
                m = half_rows * SUB

                def pixel(t, col):
                    return [src[t // 2:t // 2 + half_rows, t % 2, col, half].reshape(m, CH) for half in range(halves(l))]

                def stack(columns):
                    return jnp.concatenate([jnp.concatenate(columns(2 * q), axis=1) for q in range(J // 2)], axis=0)

                skips = []
                if kind(l) == 1:
                    for c in range(J):
                        skips.append([a_buf[g, pl.ds(r0 + 1, BC), c + 1, half].reshape(half_rows, 2, SUB, CH) for half in range(2)])

                def taps(r, q2):
                    own = []
                    for dy in range(3):
                        own += pixel(r + dy, q2 + 1) + pixel(r + dy, q2 + 2)
                    if kind(l) == 1:
                        own += [v[:, r:r + 1].reshape(m, CH) for c in range(2) for v in skips[q2 + c]]
                    corner = pixel(3 * r, q2) + pixel(3 * r, q2 + 3)
                    return own + corner if r else corner + own

                def mm(lhs, start, size):
                    return jnp.dot(lhs, wp[start:start + size, :], preferred_element_type=f32)

                rows = [mm(stack(lambda q2: taps(r, q2)), 2 * ch * r, mid + 2 * ch) for r in range(2)]
                base = mid + 4 * ch
                sides = [mm(stack(lambda q2: pixel(1, q2 + 3 * s) + pixel(2, q2 + 3 * s)), base + 2 * ch * s, 2 * ch) for s in range(2)]
                for q in range(J // 2):
                    for s in range(2):
                        pair = []
                        for r in range(2):
                            v = rows[r][q * m:(q + 1) * m, s * CH:(s + 1) * CH] + sides[s][q * m:(q + 1) * m, r * CH:(r + 1) * CH]
                            pair.append(v.reshape(half_rows, 1, SUB, CH))
                        v = jnp.concatenate(pair, axis=1).reshape(BC, SUB, CH) + bias
                        at = (g, pl.ds(r0 + 1, BC), 2 * q + s + 1, 0)
                        if kind(l) == 3:
                            v = v + out[at].astype(f32)
                        v = v.astype(bf)
                        out[at] = v
                        v = v.astype(f32)
                        one = one + jnp.sum(v, axis=0)
                        two = two + jnp.sum(v * v, axis=0)
                return one, two

            nb = R // BC
            activate(l, g, 0, act0)

            def step(i, carry):
                one, two = carry
                one, two = block(2 * i, act0, one, two)
                activate(l, g, 2 * i + 1, act1)
                one, two = block(2 * i + 1, act1, one, two)
                activate(l, g, lax.rem(2 * i + 2, nb), act0)
                return one, two

            z = jnp.zeros((SUB, CH), f32)
            one, two = lax.fori_loop(0, nb // 2, step, (z, z))
            sacc[0, 0] = one
            sacc[1, 0] = two

        nblk = R // RB

        def edge_copy(g):
            return rcopy(ps_out.at[g], ps_in.at[g], ps_s.at[g], ps_r.at[g], {"sx": px, "sy": sy})

        def head_act(g):
            def rows(step, _):
                for k in range(HR):
                    r = HR * step + k
                    t_buf[g, r, 0:J, 0] = silu(h_buf[g, r, 1:J + 1, 0].astype(f32), 0).astype(bf)
                return 0

            lax.fori_loop(0, (R + 2) // HR, rows, 0)
            for r, border in ((0, top), (R + 1, bottom)):
                t_buf[g, r, 0:J, 0] = jnp.where(border, 0.0, t_buf[g, r, 0:J, 0].astype(f32)).astype(bf)

        def head(g):
            taps = []
            for i in range(RB + 2):
                for c in range(J):
                    taps.append(jnp.concatenate([t_buf[g, RB * b + i, c, 0] for b in range(nblk)], axis=0))
            acc = jnp.dot(jnp.concatenate(taps, axis=1), wpo[...], preferred_element_type=f32)
            y_ref[g] = acc[:, 0:CH].reshape(nblk, SUB, CH)
            for part in range(nblk // J):
                total = jnp.zeros((SUB, CH), f32)
                for k in range(J):
                    b = part * J + k
                    total = total + pltpu.roll(acc[b * SUB:(b + 1) * SUB, CH:CIN], lax.rem(k - far_edge + CH, CH), 1)
                ps_out[g, part] = total
            edge_copy(g).start()

        def add_edges(g, _):
            edge_copy(g).wait()
            lane16 = lax.broadcasted_iota(jnp.int32, (SUB, CH), 1)
            mine = (lane16 < 3 * J * RB) & (lax.rem(lane16, J) == edge)
            for b in range(nblk):
                v = pltpu.roll(ps_in[g, b // J], lax.rem(edge - b % J + CH, CH), 1)
                y_ref[g, b] = y_ref[g, b] + jnp.where(mine, v, 0.0)
            return 0

        biases = bias_ref[...].astype(f32)
        bias_rows[0:7] = biases
        bias_rows[1:2] = biases[1:2] + biases[6:7]

        def layer(l):
            def phase(g, _):
                if kind(l) > 0:
                    @pl.when(g == 1)
                    def _():
                        relay_sums(l, NG - 1)

                scales(l, g)
                finish_halo(l, g)
                conv(l, g)
                push_sums(after(l), g)

                @pl.when(g > 0)
                def _():
                    relay_sums(after(l), g - 1)

                start_halo(after(l), g)
                return 0

            lax.fori_loop(0, NG, phase, 0)

        layer(0)
        layer(1)

        def resnet(k, _):
            layer((2, 2 * k + 2))
            layer((3, 2 * k + 3))
            return 0

        lax.fori_loop(0, 2, resnet, 0)
        def last(g, _):
            @pl.when(g == 1)
            def _():
                relay_sums(LAYERS - 1, NG - 1)

            scales(LAYERS - 1, g)
            finish_halo(LAYERS - 1, g)
            head_act(g)
            head(g)
            return 0

        lax.fori_loop(0, NG, last, 0)
        lax.fori_loop(0, NG, add_edges, 0)

    def to_planes(x_ref, b_ref, o_ref, ys):
        bias = b_ref[...].astype(jnp.float32)
        blocks = x_ref.shape[1]
        rows = blocks * RB
        v = x_ref[0].reshape(blocks * SUB, CH)
        for ro in range(RB):
            u = pltpu.roll(v, CH - 3 * J * ro, 1) if ro else v
            for b in range(blocks):
                ys[(RB * b + ro) * SUB:(RB * b + ro + 1) * SUB] = u[b * SUB:(b + 1) * SUB]
        for i in range(NS):
            parts = [ys[pl.ds(p * NS + i, rows, stride=SUB), :] for p in range(NG)]
            flat = jnp.transpose(jnp.concatenate(parts, axis=0))
            for c in range(3):
                o_ref[i, c] = flat[c * J:(c + 1) * J] + bias[:, c:c + 1]

    def local_decode(act_in, norm_first, w_first, w_short, norm_rest, w_rest, bias_rest, w_out, bias_out):
        n, h, w, cin = act_in.shape
        rr = h // NG
        a = act_in.reshape(n, NG, rr, w, cin)
        f32 = jnp.float32
        lanes = jnp.arange(CH)[None, None, :]
        place = (lanes == (J * jnp.arange(3)[None, :, None] + 2 - jnp.arange(3)[:, None, None])).astype(jnp.bfloat16)
        wo = jnp.einsum("yxco,xol->ycl", w_out, place, preferred_element_type=f32)
        vm = pl.BlockSpec(memory_space=pltpu.VMEM)
        bf = jnp.bfloat16
        dma = pltpu.SemaphoreType.DMA
        block_map = pltpu.VMEM((BC // 2 + 1, 2, J + 2, 2, SUB, CH), bf)
        sides = dma((LAYERS, NG, 2))
        y = pl.pallas_call(
            kernel,
            out_shape=jax.ShapeDtypeStruct((NG, rr // RB, SUB, CH), f32),
            in_specs=[pl.BlockSpec(memory_space=pl.ANY)] + [vm] * 7,
            out_specs=vm,
            scratch_shapes=[
                pltpu.VMEM((NG, rr + 2, J + 1, 2, SUB, CH), bf),
                pltpu.VMEM((NG, rr + 2, J + 1, 1, SUB, CH), bf),
                pltpu.VMEM((NG, rr + 2, J + 1, 1, SUB, CH), bf),
                pltpu.VMEM((NG, 2, J, 2, SUB, CH), bf),
                pltpu.VMEM((2, NG, 2, J, 1, SUB, CH), bf),
                pltpu.VMEM((NG, 2, 2, SUB, CH), bf),
                pltpu.VMEM((2, NG, 2, 1, SUB, CH), bf),
                block_map, block_map,
                pltpu.VMEM((TAPS * CIN, CIN), bf),
                pltpu.VMEM((TAPS * CH + 2 * CIN, CIN), bf),
                pltpu.VMEM((NG, TAPS * CH, CIN), bf),
                pltpu.VMEM(((RB + 2) * J * CH, CIN), bf),
                pltpu.VMEM((SLOTS, NS, NG, RC, J, CIN), bf),
                pltpu.VMEM((2, 2, SUB * J, CH), f32),
                pltpu.VMEM((NG, rr // RB // J, SUB, CH), f32),
                pltpu.VMEM((NG, rr // RB // J, SUB, CH), f32),
                pltpu.VMEM((8, CH), f32),
                pltpu.VMEM((2, 2, SUB, CH), f32),
                pltpu.VMEM((2, NG, 2, 8, CH), f32),
                pltpu.VMEM((2, NG, 3, 2, 8, CH), f32),
                pltpu.VMEM((2, NG, 2, 8, CH), f32),
                pltpu.VMEM((2, NG, 2, 8, CH), f32),
                pltpu.VMEM((2, 2, SUB, CH), f32),
                dma((SLOTS,)),
                dma((LAYERS, NG)), dma((LAYERS, NG)),
                sides, sides, sides, sides,
                dma((LAYERS, NG, 3)), dma((LAYERS, NG, 3)),
                dma((LAYERS, NG)), dma((LAYERS, NG)),
                dma((NG,)), dma((NG,)),
                dma((rr // RC,)), dma((rr // RC,)),
            ],
            compiler_params=pltpu.CompilerParams(collective_id=0, has_side_effects=True, vmem_limit_bytes=67043328),
            name="decode",
        )(a, w_first, w_rest, w_short, wo, norm_first, norm_rest, bias_rest)
        y = pl.pallas_call(
            to_planes,
            grid=(NG,),
            out_shape=jax.ShapeDtypeStruct((n, 3, J, h), f32),
            in_specs=[pl.BlockSpec((1, rr // RB, SUB, CH), lambda g: (g, 0, 0, 0)), pl.BlockSpec((1, 3), lambda g: (0, 0))],
            out_specs=pl.BlockSpec((NS, 3, J, h), lambda g: (g, 0, 0, 0)),
            scratch_shapes=[pltpu.VMEM((rr * SUB, CH), f32)],
            name="to_planes",
        )(y, bias_out.reshape(1, 3))
        return jnp.transpose(y, (0, 3, 2, 1))

    return jax.shard_map(local_decode, mesh=mesh, in_specs=(tile_spec,) + (rep,) * 8, out_specs=tile_spec, check_vma=False)
```

```python
import jax
import jax.numpy as jnp
from jax import lax
from jax.experimental import pallas as pl
from jax.experimental.pallas import tpu as pltpu
from jax.sharding import PartitionSpec as P

MESH = pl.DeviceIdType.MESH
GN_EPS = 1e-6
NG = 4
NS = 4
SUB = 16
J = 8
BC = 16
RC = 8
SLOTS = 4
RB = 4
HR = 6
LAYERS = 7
CH = 128
CIN = 256
TAPS = 14


def solution(mesh):
    tile_spec = P("dp", "sy", "sx", None)
    rep = P()

    def kernel(a_hbm, w1_ref, wr_ref, ws_ref, wo_ref, n0_ref, nr_ref, bias_ref, y_ref,
               a_buf, t_buf, h_buf, rowa, rowx, cora, corx, act0, act1, wp1, wp2, wpr, wpo,
               raw, tmp, ps_out, ps_in, bias_rows, sacc, st_own, st_in, st_sum, st_far, sb,
               raw_sem, col_s, col_r, row_s, row_r, cor_s, cor_r, st_s, st_r, far_s, far_r, ps_s, ps_r, pc_s, pc_r):
        sx = lax.axis_index("sx")
        sy = lax.axis_index("sy")
        px = 1 - sx
        up = lax.rem(sy + 3, 4)
        dn = lax.rem(sy + 1, 4)
        R = a_buf.shape[1] - 2
        count = 1024.0 * 16.0
        f32, bf = jnp.float32, jnp.bfloat16

        barrier = pltpu.get_barrier_semaphore()
        friends = [{"sx": sx, "sy": lax.rem(sy + d, 4)} for d in range(1, 4)]
        friends += [{"sx": px, "sy": sy}, {"sx": px, "sy": up}, {"sx": px, "sy": dn}]
        for dev in friends:
            pl.semaphore_signal(barrier, inc=1, device_id=dev, device_id_type=MESH)

        def raw_copy(g, chunk, slot):
            return pltpu.make_async_copy(
                a_hbm.at[pl.ds(g * NS, NS), :, pl.ds(chunk * RC, RC)], raw.at[slot], raw_sem.at[slot])

        nchunk = R // RC
        for ahead in range(SLOTS - 1):
            raw_copy(0, ahead, ahead).start()

        def rcopy(src, dst, ss, rs, dev):
            return pltpu.make_async_remote_copy(src_ref=src, dst_ref=dst, send_sem=ss, recv_sem=rs, device_id=dev, device_id_type=MESH)

        def kind(l):
            return l if isinstance(l, int) else l[0]

        def index(l):
            return l if isinstance(l, int) else l[1]

        def after(l):
            return l + 1 if isinstance(l, int) else (5 - l[0], l[1] + 1)

        def halves(l):
            return 2 if kind(l) == 0 else 1

        def xbuf(l):
            return a_buf if kind(l) == 0 else (t_buf if kind(l) % 2 else h_buf)

        def halo_bufs(l, g):
            if kind(l) == 0:
                return rowa.at[g], cora.at[g]
            return rowx.at[kind(l) % 2, g], corx.at[kind(l) % 2, g]

        def row_copies(l, g):
            x = xbuf(l)
            row, _ = halo_bufs(l, g)
            return [
                rcopy(x.at[g, R, pl.ds(1, J)], row.at[0], row_s.at[index(l), g, 0], row_r.at[index(l), g, 0], {"sx": sx, "sy": dn}),
                rcopy(x.at[g, 1, pl.ds(1, J)], row.at[1], row_s.at[index(l), g, 1], row_r.at[index(l), g, 1], {"sx": sx, "sy": up}),
            ]

        def piece_copy(ch):
            rows = pl.ds(ch * RC + 1, RC)
            return rcopy(a_buf.at[0, rows, 1], a_buf.at[0, rows, 0], pc_s.at[ch], pc_r.at[ch], {"sx": px, "sy": sy})

        def col_copy(l, g):
            x = xbuf(l)
            return rcopy(x.at[g, pl.ds(1, R), 1], x.at[g, pl.ds(1, R), 0], col_s.at[index(l), g], col_r.at[index(l), g], {"sx": px, "sy": sy})

        def corner_copies(l, g):
            x = xbuf(l)
            _, cor = halo_bufs(l, g)
            return [
                rcopy(x.at[g, R, 1], cor.at[0], cor_s.at[index(l), g, 0], cor_r.at[index(l), g, 0], {"sx": px, "sy": dn}),
                rcopy(x.at[g, 1, 1], cor.at[1], cor_s.at[index(l), g, 1], cor_r.at[index(l), g, 1], {"sx": px, "sy": up}),
            ]

        def start_halo(l, g):
            for c in row_copies(l, g):
                c.start()
            if kind(l) == 2:
                @pl.when(index(l) < LAYERS - 1)
                def _():
                    for c in corner_copies(l, g) + [col_copy(l, g)]:
                        c.start()
            else:
                for c in corner_copies(l, g):
                    c.start()
                if kind(l) == 0:
                    @pl.when(g > 0)
                    def _():
                        col_copy(l, g).start()
                else:
                    col_copy(l, g).start()

        def near_copies(l, g):
            nh = halves(l)
            return [
                rcopy(st_own.at[kind(l) % 2, g, pl.ds(0, nh)], st_in.at[kind(l) % 2, g, d - 1, pl.ds(0, nh)],
                      st_s.at[index(l), g, d - 1], st_r.at[index(l), g, d - 1], friends[d - 1])
                for d in range(1, 4)
            ]

        def far_copy(l, g):
            nh = halves(l)
            return rcopy(st_sum.at[kind(l) % 2, g, pl.ds(0, nh)], st_far.at[kind(l) % 2, g, pl.ds(0, nh)],
                         far_s.at[index(l), g], far_r.at[index(l), g], {"sx": px, "sy": sy})

        sub8 = lax.broadcasted_iota(jnp.int32, (8, CH), 0)
        lane8 = lax.broadcasted_iota(jnp.int32, (8, CH), 1)
        sub16 = lax.broadcasted_iota(jnp.int32, (SUB, CH), 0)

        def fold(v):
            v = v[0:8] + v[8:16]
            return v + pltpu.roll(v, 4, 0)

        def push_sums(l, g):
            for half in range(halves(l)):
                st_own[kind(l) % 2, g, half] = jnp.where(sub8 < 4, fold(sacc[0, half]), fold(sacc[1, half]))
            for c in near_copies(l, g):
                c.start()

        def relay_sums(l, g):
            for c in near_copies(l, g):
                c.wait()
            for half in range(halves(l)):
                x = st_own[kind(l) % 2, g, half]
                for d in range(3):
                    x = x + st_in[kind(l) % 2, g, d, half]
                st_sum[kind(l) % 2, g, half] = x
            far_copy(l, g).start()

        def load_group(g, _):
            sacc[...] = jnp.zeros_like(sacc)

            def load_chunk(ch, _):
                step = g * nchunk + ch
                slot = lax.rem(step, SLOTS)
                nxt = step + SLOTS - 1

                @pl.when(nxt < NG * nchunk)
                def _():
                    raw_copy(lax.div(nxt, nchunk), lax.rem(nxt, nchunk), lax.rem(nxt, SLOTS)).start()

                raw_copy(g, ch, slot).wait()
                ones = [jnp.zeros((SUB, CH), f32) for _ in range(2)]
                twos = [jnp.zeros((SUB, CH), f32) for _ in range(2)]
                for r in range(RC):
                    for p in range(NG):
                        for i in range(NS):
                            v = raw[slot, i, p, r].astype(f32)
                            base = (p * NS + i) * J
                            tmp[r % 2, 0, base:base + J, :] = v[:, :CH]
                            tmp[r % 2, 1, base:base + J, :] = v[:, CH:]
                    for w in range(J):
                        j = sx * w + (1 - sx) * (J - 1 - w)
                        for half in range(2):
                            v = tmp[r % 2, half, pl.ds(w, SUB, stride=J), :]
                            a_buf[g, ch * RC + r + 1, j + 1, half] = v.astype(bf)
                            ones[half] = ones[half] + v
                            twos[half] = twos[half] + v * v
                for half in range(2):
                    sacc[0, half] = sacc[0, half] + ones[half]
                    sacc[1, half] = sacc[1, half] + twos[half]

                @pl.when(g == 0)
                def _():
                    @pl.when(ch == 0)
                    def _():
                        pl.semaphore_wait(barrier, len(friends))

                    piece_copy(ch).start()

                return 0

            lax.fori_loop(0, nchunk, load_chunk, 0)

            push_sums(0, g)

            @pl.when(g > 0)
            def _():
                relay_sums(0, g - 1)

            start_halo(0, g)
            return 0

        lax.fori_loop(0, NG, load_group, 0)

        def fill_block(dst, w, ch, extra):
            zero = jnp.zeros((ch, CH), bf)

            def tap(dy, dx):
                return w[dy, sx * dx + (1 - sx) * (2 - dx)]

            parts = [(tap(0, 0), zero), (zero, tap(0, 2))]
            for dy in range(3):
                parts += [(tap(dy, 1), tap(dy, 0)), (tap(dy, 2), tap(dy, 1))]
            tail = [(tap(2, 0), zero), (zero, tap(2, 2))]
            for dx in (0, 2):
                tail += [(tap(1, dx), tap(0, dx)), (tap(2, dx), tap(1, dx))]
            k = 0
            for group in (parts, extra, tail):
                for left, right in group:
                    size = left.shape[0]
                    dst[k:k + size, 0:CH] = left
                    dst[k:k + size, CH:CIN] = right
                    k += size

        fill_block(wp1, w1_ref, CIN, [])
        relay_sums(0, NG - 1)
        fill_block(wp2, wr_ref.at[0], CH, [(ws_ref[...], jnp.zeros((CIN, CH), bf)), (jnp.zeros((CIN, CH), bf), ws_ref[...])])

        def fill_rest(k, _):
            fill_block(wpr.at[k - 1], wr_ref.at[k], CH, [])
            return 0

        lax.fori_loop(1, 5, fill_rest, 0)

        lane128 = lax.broadcasted_iota(jnp.int32, (CH, CH), 1)

        def place_rows(c, placed, col):
            for i in range(RB + 2):
                total = jnp.zeros((CH, CH), f32)
                for dy in range(3):
                    ro = i - dy
                    if 0 <= ro < RB:
                        total = total + (pltpu.roll(placed[dy], 3 * J * ro, 1) if ro else placed[dy])
                k = pl.multiple_of((i * J + c) * CH, CH)
                wpo[pl.ds(k, CH), col:col + CH] = total.astype(bf)

        def fill_out(c, _):
            first = sx * (c + 1) + (1 - sx) * (J - c) - 2
            tap = lax.rem(lane128, J) - first
            keep = (lane128 < 3 * J) & (tap >= 0) & (tap <= 2)
            place_rows(c, [jnp.where(keep, pltpu.roll(wo_ref[dy], lax.rem(first + CH, CH), 1), 0.0) for dy in range(3)], 0)
            for i in range(RB + 2):
                k = pl.multiple_of((i * J + c) * CH, CH)
                wpo[pl.ds(k, CH), CH:CIN] = jnp.zeros((CH, CH), bf)
            return 0

        lax.fori_loop(0, J, fill_out, 0)
        edge = (J - 1) * (1 - sx)
        far_edge = (J - 1) * sx
        keep = (lane128 < 3 * J) & (lax.rem(lane128, J) == far_edge)
        place_rows(0, [jnp.where(keep, pltpu.roll(wo_ref[dy], lax.rem(far_edge - 2 * (1 - sx) + CH, CH), 1), 0.0) for dy in range(3)], CH)

        for block_map in (act0, act1):
            block_map[:, :, J + 1] = jnp.zeros((BC // 2 + 1, 2, 2, SUB, CH), bf)

        def scales(l, g):
            per = 8 if kind(l) == 0 else 4
            far_copy(l, g).wait()
            for half in range(halves(l)):
                x = st_sum[kind(l) % 2, g, half] + st_far[kind(l) % 2, g, half]
                k = 1
                while k < per:
                    x = x + jnp.where((lane8 & k) == 0, pltpu.roll(x, CH - k, 1), pltpu.roll(x, k, 1))
                    k *= 2
                flip = pltpu.roll(x, 4, 0)
                mean = jnp.where(sub8 < 4, x, flip) / (count * per)
                var = jnp.where(sub8 < 4, flip, x) / (count * per) - mean * mean
                if kind(l) == 0:
                    pair = n0_ref[:, half * CH:(half + 1) * CH].astype(f32)
                else:
                    pair = nr_ref[index(l) - 1].astype(f32)
                s = lax.rsqrt(var + GN_EPS) * pair[0:1]
                b = pair[1:2] - mean * s
                sb[0, half] = 0.5 * jnp.concatenate([s, s], axis=0)
                sb[1, half] = 0.5 * jnp.concatenate([b, b], axis=0)

        def finish_halo(l, g):
            x = xbuf(l)
            last = kind(l) == LAYERS - 1
            for c in row_copies(l, g):
                c.wait()
            if not last:
                for c in corner_copies(l, g):
                    c.wait()
            if kind(l) == 0:
                @pl.when(g == 0)
                def _():
                    for ch in range(nchunk):
                        piece_copy(ch).wait()

                @pl.when(g > 0)
                def _():
                    col_copy(l, g).wait()
            elif not last:
                col_copy(l, g).wait()
            row, cor = halo_bufs(l, g)
            for side in range(2):
                shift = NS if side == 0 else SUB - NS
                outer = (sub16 < NS) if side == 0 else (sub16 >= SUB - NS)
                for j in range(1 if last else 0, J + 1):
                    for half in range(halves(l)):
                        own = x[g, R if side == 0 else 1, j, half].astype(f32)
                        far = (row[side, j - 1, half] if j else cor[side, half]).astype(f32)
                        v = jnp.where(outer, pltpu.roll(far, shift, 0), pltpu.roll(own, shift, 0))
                        x[g, 0 if side == 0 else R + 1, j, half] = v.astype(bf)

        def silu(x, half):
            u = x * sb[0, half] + sb[1, half]
            return u + u * jnp.tanh(u)

        top = (sub16 < NS) & (sy == 0)
        bottom = (sub16 >= SUB - NS) & (sy == 3)

        def activate(l, g, b, dst):
            x = xbuf(l)
            nb = R // BC
            for i in range(BC + 2):
                for half in range(halves(l)):
                    v = silu(x[g, b * BC + i, :, half].astype(f32), half)
                    if i == 0:
                        v = jnp.where(top & (b == 0), 0.0, v)
                    if i == BC + 1:
                        v = jnp.where(bottom & (b == nb - 1), 0.0, v)
                    dst[i // 2, i % 2, 0:J + 1, half] = v.astype(bf)

        def conv(l, g):
            wp = wp1 if kind(l) == 0 else (wp2 if kind(l) == 1 else wpr.at[index(l) - 2])
            out = xbuf(after(l))
            bias = bias_rows[pl.ds(index(l), 1), :]
            bias = jnp.broadcast_to(bias.reshape(1, 1, CH), (BC, SUB, CH))

            half_rows = BC // 2
            ch = CH * halves(l)
            mid = 6 * ch + (2 * CIN if kind(l) == 1 else 0)

            def block(b, src, one, two):
                r0 = b * BC
                m = half_rows * SUB

                def pixel(t, col):
                    return [src[t // 2:t // 2 + half_rows, t % 2, col, half].reshape(m, CH) for half in range(halves(l))]

                def stack(columns):
                    return jnp.concatenate([jnp.concatenate(columns(2 * q), axis=1) for q in range(J // 2)], axis=0)

                skips = []
                if kind(l) == 1:
                    for c in range(J):
                        skips.append([a_buf[g, pl.ds(r0 + 1, BC), c + 1, half].reshape(half_rows, 2, SUB, CH) for half in range(2)])

                def taps(r, q2):
                    own = []
                    for dy in range(3):
                        own += pixel(r + dy, q2 + 1) + pixel(r + dy, q2 + 2)
                    if kind(l) == 1:
                        own += [v[:, r:r + 1].reshape(m, CH) for c in range(2) for v in skips[q2 + c]]
                    corner = pixel(3 * r, q2) + pixel(3 * r, q2 + 3)
                    return own + corner if r else corner + own

                def mm(lhs, start, size):
                    return jnp.dot(lhs, wp[start:start + size, :], preferred_element_type=f32)

                rows = [mm(stack(lambda q2: taps(r, q2)), 2 * ch * r, mid + 2 * ch) for r in range(2)]
                base = mid + 4 * ch
                sides = [mm(stack(lambda q2: pixel(1, q2 + 3 * s) + pixel(2, q2 + 3 * s)), base + 2 * ch * s, 2 * ch) for s in range(2)]
                for q in range(J // 2):
                    for s in range(2):
                        pair = []
                        for r in range(2):
                            v = rows[r][q * m:(q + 1) * m, s * CH:(s + 1) * CH] + sides[s][q * m:(q + 1) * m, r * CH:(r + 1) * CH]
                            pair.append(v.reshape(half_rows, 1, SUB, CH))
                        v = jnp.concatenate(pair, axis=1).reshape(BC, SUB, CH) + bias
                        at = (g, pl.ds(r0 + 1, BC), 2 * q + s + 1, 0)
                        if kind(l) == 3:
                            v = v + out[at].astype(f32)
                        v = v.astype(bf)
                        out[at] = v
                        v = v.astype(f32)
                        one = one + jnp.sum(v, axis=0)
                        two = two + jnp.sum(v * v, axis=0)
                return one, two

            nb = R // BC
            activate(l, g, 0, act0)

            def step(i, carry):
                one, two = carry
                one, two = block(2 * i, act0, one, two)
                activate(l, g, 2 * i + 1, act1)
                one, two = block(2 * i + 1, act1, one, two)
                activate(l, g, lax.rem(2 * i + 2, nb), act0)
                return one, two

            z = jnp.zeros((SUB, CH), f32)
            one, two = lax.fori_loop(0, nb // 2, step, (z, z))
            sacc[0, 0] = one
            sacc[1, 0] = two

        nblk = R // RB

        def edge_copy(g):
            return rcopy(ps_out.at[g], ps_in.at[g], ps_s.at[g], ps_r.at[g], {"sx": px, "sy": sy})

        def head_act(g):
            def rows(step, _):
                for k in range(HR):
                    r = HR * step + k
                    t_buf[g, r, 0:J, 0] = silu(h_buf[g, r, 1:J + 1, 0].astype(f32), 0).astype(bf)
                return 0

            lax.fori_loop(0, (R + 2) // HR, rows, 0)
            for r, border in ((0, top), (R + 1, bottom)):
                t_buf[g, r, 0:J, 0] = jnp.where(border, 0.0, t_buf[g, r, 0:J, 0].astype(f32)).astype(bf)

        def head(g):
            taps = []
            for i in range(RB + 2):
                for c in range(J):
                    taps.append(jnp.concatenate([t_buf[g, RB * b + i, c, 0] for b in range(nblk)], axis=0))
            acc = jnp.dot(jnp.concatenate(taps, axis=1), wpo[...], preferred_element_type=f32)
            y_ref[g] = acc[:, 0:CH].reshape(nblk, SUB, CH)
            for part in range(nblk // J):
                total = jnp.zeros((SUB, CH), f32)
                for k in range(J):
                    b = part * J + k
                    total = total + pltpu.roll(acc[b * SUB:(b + 1) * SUB, CH:CIN], lax.rem(k - far_edge + CH, CH), 1)
                ps_out[g, part] = total
            edge_copy(g).start()

        def add_edges(g, _):
            edge_copy(g).wait()
            lane16 = lax.broadcasted_iota(jnp.int32, (SUB, CH), 1)
            mine = (lane16 < 3 * J * RB) & (lax.rem(lane16, J) == edge)
            for b in range(nblk):
                v = pltpu.roll(ps_in[g, b // J], lax.rem(edge - b % J + CH, CH), 1)
                y_ref[g, b] = y_ref[g, b] + jnp.where(mine, v, 0.0)
            return 0

        biases = bias_ref[...].astype(f32)
        bias_rows[0:7] = biases
        bias_rows[1:2] = biases[1:2] + biases[6:7]

        def layer(l):
            def phase(g, _):
                if kind(l) > 0:
                    @pl.when(g == 1)
                    def _():
                        relay_sums(l, NG - 1)

                scales(l, g)
                finish_halo(l, g)
                conv(l, g)
                start_halo(after(l), g)
                push_sums(after(l), g)

                @pl.when(g > 0)
                def _():
                    relay_sums(after(l), g - 1)

                return 0

            lax.fori_loop(0, NG, phase, 0)

        layer(0)
        layer(1)

        def resnet(k, _):
            layer((2, 2 * k + 2))
            layer((3, 2 * k + 3))
            return 0

        lax.fori_loop(0, 2, resnet, 0)
        def last(g, _):
            @pl.when(g == 1)
            def _():
                relay_sums(LAYERS - 1, NG - 1)

            scales(LAYERS - 1, g)
            finish_halo(LAYERS - 1, g)
            head_act(g)
            head(g)
            return 0

        lax.fori_loop(0, NG, last, 0)
        lax.fori_loop(0, NG, add_edges, 0)

    def to_planes(x_ref, b_ref, o_ref, ys):
        bias = b_ref[...].astype(jnp.float32)
        blocks = x_ref.shape[1]
        rows = blocks * RB
        v = x_ref[0].reshape(blocks * SUB, CH)
        for ro in range(RB):
            u = pltpu.roll(v, CH - 3 * J * ro, 1) if ro else v
            for b in range(blocks):
                ys[(RB * b + ro) * SUB:(RB * b + ro + 1) * SUB] = u[b * SUB:(b + 1) * SUB]
        for i in range(NS):
            parts = [ys[pl.ds(p * NS + i, rows, stride=SUB), :] for p in range(NG)]
            flat = jnp.transpose(jnp.concatenate(parts, axis=0))
            for c in range(3):
                o_ref[i, c] = flat[c * J:(c + 1) * J] + bias[:, c:c + 1]

    def local_decode(act_in, norm_first, w_first, w_short, norm_rest, w_rest, bias_rest, w_out, bias_out):
        n, h, w, cin = act_in.shape
        rr = h // NG
        a = act_in.reshape(n, NG, rr, w, cin)
        f32 = jnp.float32
        lanes = jnp.arange(CH)[None, None, :]
        place = (lanes == (J * jnp.arange(3)[None, :, None] + 2 - jnp.arange(3)[:, None, None])).astype(jnp.bfloat16)
        wo = jnp.einsum("yxco,xol->ycl", w_out, place, preferred_element_type=f32)
        vm = pl.BlockSpec(memory_space=pltpu.VMEM)
        bf = jnp.bfloat16
        dma = pltpu.SemaphoreType.DMA
        block_map = pltpu.VMEM((BC // 2 + 1, 2, J + 2, 2, SUB, CH), bf)
        sides = dma((LAYERS, NG, 2))
        y = pl.pallas_call(
            kernel,
            out_shape=jax.ShapeDtypeStruct((NG, rr // RB, SUB, CH), f32),
            in_specs=[pl.BlockSpec(memory_space=pl.ANY)] + [vm] * 7,
            out_specs=vm,
            scratch_shapes=[
                pltpu.VMEM((NG, rr + 2, J + 1, 2, SUB, CH), bf),
                pltpu.VMEM((NG, rr + 2, J + 1, 1, SUB, CH), bf),
                pltpu.VMEM((NG, rr + 2, J + 1, 1, SUB, CH), bf),
                pltpu.VMEM((NG, 2, J, 2, SUB, CH), bf),
                pltpu.VMEM((2, NG, 2, J, 1, SUB, CH), bf),
                pltpu.VMEM((NG, 2, 2, SUB, CH), bf),
                pltpu.VMEM((2, NG, 2, 1, SUB, CH), bf),
                block_map, block_map,
                pltpu.VMEM((TAPS * CIN, CIN), bf),
                pltpu.VMEM((TAPS * CH + 2 * CIN, CIN), bf),
                pltpu.VMEM((NG, TAPS * CH, CIN), bf),
                pltpu.VMEM(((RB + 2) * J * CH, CIN), bf),
                pltpu.VMEM((SLOTS, NS, NG, RC, J, CIN), bf),
                pltpu.VMEM((2, 2, SUB * J, CH), f32),
                pltpu.VMEM((NG, rr // RB // J, SUB, CH), f32),
                pltpu.VMEM((NG, rr // RB // J, SUB, CH), f32),
                pltpu.VMEM((8, CH), f32),
                pltpu.VMEM((2, 2, SUB, CH), f32),
                pltpu.VMEM((2, NG, 2, 8, CH), f32),
                pltpu.VMEM((2, NG, 3, 2, 8, CH), f32),
                pltpu.VMEM((2, NG, 2, 8, CH), f32),
                pltpu.VMEM((2, NG, 2, 8, CH), f32),
                pltpu.VMEM((2, 2, SUB, CH), f32),
                dma((SLOTS,)),
                dma((LAYERS, NG)), dma((LAYERS, NG)),
                sides, sides, sides, sides,
                dma((LAYERS, NG, 3)), dma((LAYERS, NG, 3)),
                dma((LAYERS, NG)), dma((LAYERS, NG)),
                dma((NG,)), dma((NG,)),
                dma((rr // RC,)), dma((rr // RC,)),
            ],
            compiler_params=pltpu.CompilerParams(collective_id=0, has_side_effects=True, vmem_limit_bytes=67043328),
            name="decode",
        )(a, w_first, w_rest, w_short, wo, norm_first, norm_rest, bias_rest)
        y = pl.pallas_call(
            to_planes,
            grid=(NG,),
            out_shape=jax.ShapeDtypeStruct((n, 3, J, h), f32),
            in_specs=[pl.BlockSpec((1, rr // RB, SUB, CH), lambda g: (g, 0, 0, 0)), pl.BlockSpec((1, 3), lambda g: (0, 0))],
            out_specs=pl.BlockSpec((NS, 3, J, h), lambda g: (g, 0, 0, 0)),
            scratch_shapes=[pltpu.VMEM((rr * SUB, CH), f32)],
            name="to_planes",
        )(y, bias_out.reshape(1, 3))
        return jnp.transpose(y, (0, 3, 2, 1))

    return jax.shard_map(local_decode, mesh=mesh, in_specs=(tile_spec,) + (rep,) * 8, out_specs=tile_spec, check_vma=False)
```
